256 devices in a mesh: band: 16 (over y_lo, z), dom: 16 (over x, y_hi, core).
Axes of the slice: x: 4, y: 4 (y_hi: 2, y_lo: 2; y = y_hi * 2 + y_lo), z: 8, core: 2. Of those that a mesh axis runs over, the one named last changes fastest.
Arguments:
- wavefunctions: float32 [1024, 64, 16, 128], P('band', 'dom'), may hold values from -6 to 6
- potential: float32 [64, 16, 128], P('dom'), may hold values from -40 to 40
- projectors: float32 [64, 18, 4, 16, 128], P('dom'), may hold values from -0.0625 to 0.0625
- hamiltonian_correction: float32 [64, 18, 18], P('dom'), may hold values from -0.0390625 to 0.0390625
- delta_s: float32 [64, 18, 18], P('dom'), may hold values from -0.0390625 to 0.0390625
- projector_count: int32 [64], P('dom'), may hold values from 1 to 18
Outputs:
- ham: float32 [1024, 1024], P('band')
- correlation: float32 [1024, 1024], P('band')
The draws below stay inside these ranges and needn't reach their ends.
All inputs are finite; a program needn't handle non-finite values.
Results may differ from the reference program's by a relative error of at most 0.00007.
Values sent between devices are 32-bit elements; how exact they have to be, the bound alone decides.
No kernel may reach another device: no remote copies, remote signals or barrier semaphores. Data moves between devices by JAX's collectives and lax.ppermute only.
A program may use at most 192 MiB of HBM per device.

```python
import jax
import jax.numpy as jnp
from jax import lax

BANDS = 1024
NPROJ = 18
A_DEV = 4
CX = 4
NY = 16
NZ = 128
NX = 64
ATOMS = 64
N_DOM = 16


def place_ends(entries, rng, least, largest):
    extent = entries.shape
    index_at = [jax.random.randint(jax.random.fold_in(rng, axis), (), 0, extent[axis]) for axis in range(len(extent))]
    entries = entries.at[tuple(index_at)].set(least)
    longest = extent.index(max(extent))
    index_at[longest] = (index_at[longest] + 1) % extent[longest]
    return entries.at[tuple(index_at)].set(largest)


def block_levels(rng, dims, pieces, least, top_value):
    gain = 1.0
    for axis_at, parts in pieces:
        heights = jax.random.uniform(jax.random.fold_in(jax.random.fold_in(rng, 6), axis_at), (parts,), jnp.float32, least / len(pieces), top_value / len(pieces))
        gain = gain * jnp.repeat(jnp.exp(heights), dims[axis_at] // parts).reshape((-1,) + (1,) * (len(dims) - 1 - axis_at))
    return gain


def centred(stream_key, shape, deviation, reach, cuts=(), kind=jnp.bfloat16):
    result = deviation * jax.random.normal(stream_key, shape, jnp.float32)
    if cuts:
        result = result * block_levels(stream_key, shape, cuts, -0.22, 0.18)
    return jnp.clip(result, -reach, reach).astype(kind)


def setup_inputs(seed: int = 0) -> dict:
    arg_keys = jax.random.split(jax.random.key(seed), 7)
    return {
        "wavefunctions": centred(arg_keys[0], (BANDS, NX, NY, NZ), 1.0, 6.0, ((0, 16), (1, 16)), jnp.float32),
        "potential": jnp.clip(jax.random.uniform(arg_keys[1], (NX, NY, NZ), jnp.float32, -40.0, 40.0) * block_levels(arg_keys[1], (NX, NY, NZ), ((0, 16),), -0.4, 0.0), -40.0, 40.0),
        "projectors": centred(arg_keys[2], (ATOMS, NPROJ, CX, NY, NZ), (CX * NY * NZ) ** -0.5, 0.0625, ((0, 16),), jnp.float32),
        "hamiltonian_correction": centred(arg_keys[3], (ATOMS, NPROJ, NPROJ), (ATOMS * NPROJ * NPROJ) ** -0.5, 0.0390625, ((0, 16),), jnp.float32),
        "delta_s": centred(arg_keys[4], (ATOMS, NPROJ, NPROJ), (ATOMS * NPROJ * NPROJ) ** -0.5, 0.0390625, ((0, 16),), jnp.float32),
        "projector_count": place_ends(jax.random.randint(arg_keys[5], (ATOMS,), 1, NPROJ + 1), jax.random.fold_in(arg_keys[5], 1), 1, NPROJ).astype(jnp.int32),
    }


def rows_product(left, right):
    return lax.dot_general(left, right, (((1,), (1,)), ((), ())), precision=lax.Precision.HIGHEST, preferred_element_type=jnp.float32)


def reference(wavefunctions, potential, projectors, hamiltonian_correction, delta_s, projector_count):
    bands = wavefunctions.shape[0]
    beside = jnp.roll(wavefunctions, 1, 1) + jnp.roll(wavefunctions, -1, 1)
    beside = beside + jnp.roll(wavefunctions, 1, 2) + jnp.roll(wavefunctions, -1, 2)
    beside = beside + jnp.roll(wavefunctions, 1, 3) + jnp.roll(wavefunctions, -1, 3)
    hpsi = 0.5 * (6.0 * wavefunctions - beside) + potential[None] * wavefunctions
    volume = 1.0 / (NX * NY * NZ)
    local_cells = CX * NY * NZ
    split_psi = wavefunctions.reshape(bands, N_DOM, local_cells)
    split_proj = projectors.reshape(N_DOM, A_DEV * NPROJ, local_cells)
    projector_coefficient = jnp.einsum("bdg,dkg->bdk", split_psi, split_proj, precision=lax.Precision.HIGHEST)
    slot_mask = (jnp.arange(NPROJ, dtype=jnp.int32)[None, :] < projector_count[:, None]).astype(jnp.float32)
    projector_coefficient = projector_coefficient.reshape(bands, ATOMS, NPROJ) * slot_mask[None]
    sym_h = 0.5 * (hamiltonian_correction + jnp.swapaxes(hamiltonian_correction, 1, 2))
    sym_s = 0.5 * (delta_s + jnp.swapaxes(delta_s, 1, 2))
    coupled_h = jnp.einsum("bap,apq->baq", projector_coefficient, sym_h, precision=lax.Precision.HIGHEST).reshape(bands, -1)
    coupled_s = jnp.einsum("bap,apq->baq", projector_coefficient, sym_s, precision=lax.Precision.HIGHEST).reshape(bands, -1)
    coef_flat = projector_coefficient.reshape(bands, -1)
    psi_flat = wavefunctions.reshape(bands, -1)
    hpsi_flat = hpsi.reshape(bands, -1)
    ham = volume * rows_product(hpsi_flat, psi_flat) + rows_product(coupled_h, coef_flat)
    correlation = volume * rows_product(psi_flat, psi_flat) + rows_product(coupled_s, coef_flat)
    return ham, correlation
```

```python
import jax
import jax.numpy as jnp
from jax import lax
from jax.experimental import pallas as pl
from jax.experimental.pallas import tpu as pltpu
from jax.sharding import PartitionSpec as P

F32 = jnp.float32
BF16 = jnp.bfloat16
HI = lax.Precision.HIGHEST
VMEM = pl.BlockSpec(memory_space=pltpu.VMEM)
SMEM = pl.BlockSpec(memory_space=pltpu.SMEM)
PARAMS = pltpu.CompilerParams(vmem_limit_bytes=56 * 1024 * 1024)

SLOT_LANES = (4, 28)


def lane_of(shape):
    return lax.broadcasted_iota(jnp.int32, shape, len(shape) - 1)


def spread_kernel(wf, coef, wh, ws, out):
    lane = lane_of((8, 128))
    block = lane // 8

    def body(bg, _):
        rows = pl.ds(pl.multiple_of(bg * 8, 8), 8)
        for x in range(4):
            v = [wf[pl.ds(bg * 512 + x * 16 + y, 8, stride=64), :] for y in range(16)]
            for s in (1, 2, 4, 8):
                low = (block & s) == 0
                nxt = list(v)
                for y in range(16):
                    if not y & s:
                        a, b = v[y], v[y + s]
                        nxt[y] = jnp.where(low, a, pltpu.roll(b, s * 8, 1))
                        nxt[y + s] = jnp.where(low, pltpu.roll(a, 128 - s * 8, 1), b)
                v = nxt
            for k in range(16):
                out[k, rows, x * 128 : (x + 1) * 128] = v[k]
        cs, hs, ss = coef[rows, :], wh[rows, :], ws[rows, :]
        for k in range(16):
            acc = jnp.zeros((8, 128), F32)
            for x in range(4):
                w = out[(k + 1) % 16, rows, x * 128 : (x + 1) * 128]
                acc = jnp.where(lane % 8 == x, pltpu.roll(w, x, 1) if x else w, acc)
            for first, at in ((4 * k, 4),) + (((64 + 4 * k, 28),) if k < 2 else ()):
                for t, a in enumerate((cs, hs, ss)):
                    to = at + 8 * t
                    here = (lane >= to) & (lane < to + 4)
                    acc = jnp.where(here, pltpu.roll(a, (to - first) % 128, 1), acc)
            out[k, rows, 512:640] = acc
        return 0

    lax.fori_loop(0, 8, body, 0)


def split(x):
    hi = x.astype(BF16)
    return hi, (x - hi.astype(F32)).astype(BF16)


def gram_kernel(core, r, xh, pot, keep, send, ah, al, ph, pll, eh, es, er, c, sd):
    cells = ah.shape[1]
    volume = 1.0 / (cells * 256)
    rows_per = 64
    lane = lane_of((rows_per, 128))
    slot = (lane % 8 >= 4) & ((lane < 8) | ((lane >= 28) & (lane < 32)))

    def prepare(i, _):
        rows = pl.ds(pl.multiple_of(i * rows_per, rows_per), rows_per)
        ext = r[rows, 512:640]
        for x in range(4):
            cols = slice(x * 128, (x + 1) * 128)
            p = r[rows, cols]
            beside = r[rows, (x + 1) * 128 : (x + 2) * 128] if x < 3 else xh[rows, :]
            beside = beside + pltpu.roll(p, 120, 1)
            zn = jnp.where(lane % 8 == 7, pltpu.roll(ext, 7 - x, 1), pltpu.roll(p, 127, 1))
            beside = beside + zn
            phi = (1.5 + 0.5 * pot[x : x + 1, :]) * p - 0.5 * beside
            ah[rows, cols], al[rows, cols] = split(p)
            ph[rows, cols], pll[rows, cols] = split(phi * volume)
        zero = jnp.zeros_like(ext)
        chi, clo = [a.astype(F32) for a in split(jnp.where(slot, ext, zero))]
        er[rows, :] = (chi + pltpu.roll(clo, 8, 1) + pltpu.roll(chi, 16, 1)).astype(BF16)
        for t, e in ((1, eh), (2, es)):
            hi, lo = [a.astype(F32) for a in split(jnp.where(slot, pltpu.roll(ext, 128 - 8 * t, 1), zero))]
            e[rows, :] = (hi + pltpu.roll(hi, 8, 1) + pltpu.roll(lo, 16, 1)).astype(BF16)
        return 0

    lax.fori_loop(0, 16, prepare, 0)

    def dot(a, b):
        return lax.dot_general(a, b, (((1,), (1,)), ((), ())), preferred_element_type=F32)

    def block(t, _):
        bi, bj = t // 4, t % 4
        ri = pl.ds(pl.multiple_of(bi * 256, 256), 256)
        rj = pl.ds(pl.multiple_of(bj * 256, 256), 256)

        def ham():
            acc = dot(ph[ri, :], ah[rj, :]) + dot(ph[ri, :], al[rj, :]) + dot(pll[ri, :], ah[rj, :])
            acc += dot(ah[ri, :], ph[rj, :]) + dot(al[ri, :], ph[rj, :]) + dot(ah[ri, :], pll[rj, :])
            return acc + dot(eh[ri, :], er[rj, :])

        def corr():
            acc = dot(ah[ri, :], ah[rj, :]) + dot(ah[ri, :], al[rj, :]) + dot(al[ri, :], ah[rj, :])
            return acc * volume + dot(es[ri, :], er[rj, :])

        @pl.when(bi < bj)
        def _():
            c[bi * 4 + bj] = ham()

        @pl.when(bi > bj)
        def _():
            c[bi * 4 + bj] = corr()

        @pl.when(bi == bj)
        def _():
            s = corr()
            sd[bi] = s
            g = lax.broadcasted_iota(jnp.int32, (256, 256), 0) // 64
            h = lax.broadcasted_iota(jnp.int32, (256, 256), 1) // 64
            c[bi * 4 + bj] = jnp.where(g <= h, ham(), s)

        return 0

    lax.fori_loop(0, 16, block, 0)

    low = lane < 64
    even_here = core[0] == 0

    def tile(g, h):
        return c[(g // 4) * 4 + h // 4, (g % 4) * 64 : (g % 4) * 64 + 64, (h % 4) * 64 : (h % 4) * 64 + 128]

    def own(g):
        at = (g % 4) * 64
        return sd[g // 4, at : at + 64, at // 128 * 128 : at // 128 * 128 + 128]

    def put(e, m, even, odd):
        keep[e, m] = jnp.where(even_here, even, odd)
        send[e, m] = jnp.where(even_here, odd, even)

    for e in range(8):
        for m in range(8):
            h0, h1 = (2 * e - 2 * m) % 16, (2 * e - 2 * m - 2) % 16
            t0, t1 = tile(2 * m, h0), tile(2 * m + 1, h0)
            even = jnp.where(low, t0, tile(2 * m + 1, h1))
            odd = pltpu.roll(jnp.where(low, t1, t0), 64, 1)
            put(e, m, even, odd)
        a, b = own(e), own(e + 8)
        if e % 2:
            a = pltpu.roll(a, 64, 1)
        else:
            b = pltpu.roll(b, 64, 1)
        extra = jnp.where(low, a, b)
        put(e, 8, extra, jnp.zeros_like(extra))


def rows_kernel(dom, parts, out, total):
    d = dom[0]
    low = lane_of((64, 128)) < 64
    for m in range(9):
        acc = parts[0, m]
        for s in range(1, 8):
            acc = acc + parts[s, m]
        total[m] = acc

    def swap(x):
        return pltpu.roll(x, 64, 1)

    for g in range(16):
        h = lax.rem(d - g + 16, 16)
        left = total[g // 2] if g % 2 == 0 else swap(total[g // 2])
        other = total[h // 2]
        right = jnp.where(h % 2 == 1, other, swap(other))
        own = total[8] if g >= 8 else swap(total[8])
        out[g] = jnp.where(low, left, jnp.where(h == g, own, right))


def finish_kernel(where, parts, out):
    b, h = where[0], where[1]
    t = parts[0]
    for s in range(1, 16):
        t = t + parts[s]
    low = lane_of((64, 128)) < 64
    flipped = jnp.concatenate([t, t], axis=0).T[64:, :]
    upper = jnp.where(low, t, flipped)
    lower = jnp.where(low, flipped, pltpu.roll(t, 64, 1))
    out[...] = jnp.where(b < h, upper, jnp.where(b > h, lower, t))


def assemble_kernel(band, parts, ham, corr):
    b = band[0]
    low = lane_of((64, 128)) < 64
    for j in range(8):
        t0 = parts[lax.rem(2 * j + b, 16)]
        t1 = parts[lax.rem(2 * j + 1 + b, 16)]
        cols = slice(j * 128, (j + 1) * 128)
        ham[:, cols] = jnp.where(low, t0, pltpu.roll(t1, 64, 1))
        corr[:, cols] = jnp.where(low, pltpu.roll(t0, 64, 1), t1)


def call(kernel, args, outs, scratch=(), flops=0):
    specs = [SMEM if a.dtype == jnp.int32 else VMEM for a in args]
    size = sum(a.size * 4 for a in args) + sum(o.size * 4 for o in outs)
    single = len(outs) == 1
    return pl.pallas_call(
        kernel,
        out_shape=outs[0] if single else outs,
        in_specs=specs,
        out_specs=VMEM if single else [VMEM] * len(outs),
        scratch_shapes=scratch,
        compiler_params=PARAMS,
        cost_estimate=pl.CostEstimate(flops=flops or size, bytes_accessed=size, transcendentals=0),
    )(*args)


def shape(*dims):
    return jax.ShapeDtypeStruct(dims, F32)


def rows_product(left, right):
    return lax.dot_general(left, right, (((1,), (1,)), ((), ())), precision=HI, preferred_element_type=F32)


def on_device(wavefunctions, potential, projectors, hamiltonian_correction, delta_s, projector_count):
    bands, cx, ny, nz = wavefunctions.shape
    atoms, slots = hamiltonian_correction.shape[:2]
    b, d = lax.axis_index("band"), lax.axis_index("dom")
    scalar = lambda *v: jnp.stack([jnp.asarray(x, jnp.int32) for x in v])

    mask = (jnp.arange(slots, dtype=jnp.int32)[None, :] < projector_count[:, None]).astype(F32).reshape(-1)
    proj = projectors.reshape(atoms * slots, cx * ny * nz)
    coef = rows_product(wavefunctions.reshape(bands, cx * ny * nz), proj) * mask[None, :]
    coef = jnp.pad(coef, ((0, 0), (0, 128 - atoms * slots)))

    def coupled(m):
        m = 0.5 * (m + jnp.swapaxes(m, 1, 2))
        full = jnp.eye(atoms, dtype=F32)[:, None, :, None] * m[:, :, None, :]
        full = full.reshape(atoms * slots, atoms * slots)
        full = jnp.pad(full, (0, 128 - atoms * slots))
        return jnp.dot(coef, full, precision=HI, preferred_element_type=F32)

    wh, ws = coupled(hamiltonian_correction), coupled(delta_s)
    parts = call(spread_kernel, (wavefunctions.reshape(bands * cx * ny, nz), coef, wh, ws), (shape(16, bands, 640),))
    slab = lax.all_to_all(parts, "band", 0, 0, tiled=True).reshape(16 * bands, 640)
    ahead = lax.ppermute(slab[:, :128], "dom", [((i + 1) % 16, i) for i in range(16)])
    pot = lax.dynamic_slice_in_dim(potential, b * 8, 8, 2).reshape(cx, ny * 8)
    m = 16 * bands
    keep, send = call(
        gram_kernel,
        (scalar(d % 2), slab, ahead, pot),
        (shape(8, 9, 64, 128), shape(8, 9, 64, 128)),
        [pltpu.VMEM((m, 512), BF16)] * 4
        + [pltpu.VMEM((m, 128), BF16)] * 3
        + [pltpu.VMEM((16, 256, 256), F32), pltpu.VMEM((4, 256, 256), F32)],
        flops=9 * 2 * m * m * 512,
    )
    mate = lax.ppermute(send, "dom", [(i, i ^ 1) for i in range(16)])
    groups = [[2 * e + c for e in range(8)] for c in range(2)]
    parts = lax.all_to_all(keep + mate, "dom", 0, 0, tiled=True, axis_index_groups=groups)
    parts = call(rows_kernel, (scalar(d), parts), (shape(16, 64, 128),), [pltpu.VMEM((9, 64, 128), F32)])
    parts = lax.all_to_all(parts, "band", 0, 0, tiled=True)
    own = call(finish_kernel, (scalar(b, (d - b + 16) % 16), parts), (shape(64, 128),))
    parts = lax.all_to_all(jnp.broadcast_to(own[None], (16, 64, 128)), "dom", 0, 0, tiled=True)
    return call(assemble_kernel, (scalar(b), parts), (shape(64, 1024), shape(64, 1024)))


def solution(mesh):
    placed = (
        P("band", "dom", None, None),
        P("dom", None, None),
        P("dom", None, None, None, None),
        P("dom", None, None),
        P("dom", None, None),
        P("dom"),
    )
    return jax.shard_map(
        on_device,
        mesh=mesh,
        in_specs=placed,
        out_specs=(P("band", None), P("band", None)),
        check_vma=False,
    )
```

```python
import jax
import jax.numpy as jnp
from jax import lax
from jax.experimental import pallas as pl
from jax.experimental.pallas import tpu as pltpu
from jax.sharding import PartitionSpec as P

F32 = jnp.float32
BF16 = jnp.bfloat16
HI = lax.Precision.HIGHEST
VMEM = pl.BlockSpec(memory_space=pltpu.VMEM)
SMEM = pl.BlockSpec(memory_space=pltpu.SMEM)

SLOT_LANES = (4, 28)


def lane_of(shape):
    return lax.broadcasted_iota(jnp.int32, shape, len(shape) - 1)


def spread_kernel(wf, coef, wh, ws, out):
    lane = lane_of((8, 128))
    block = lane // 8

    def body(bg, _):
        rows = pl.ds(pl.multiple_of(bg * 8, 8), 8)
        for x in range(4):
            v = [wf[pl.ds(bg * 512 + x * 16 + y, 8, stride=64), :] for y in range(16)]
            for s in (1, 2, 4, 8):
                low = (block & s) == 0
                nxt = list(v)
                for y in range(16):
                    if not y & s:
                        a, b = v[y], v[y + s]
                        nxt[y] = jnp.where(low, a, pltpu.roll(b, s * 8, 1))
                        nxt[y + s] = jnp.where(low, pltpu.roll(a, 128 - s * 8, 1), b)
                v = nxt
            for k in range(16):
                out[k, rows, x * 128 : (x + 1) * 128] = v[k]
        cs, hs, ss = coef[rows, :], wh[rows, :], ws[rows, :]
        for k in range(16):
            acc = jnp.zeros((8, 128), F32)
            for x in range(4):
                w = out[(k + 1) % 16, rows, x * 128 : (x + 1) * 128]
                acc = jnp.where(lane % 8 == x, pltpu.roll(w, x, 1) if x else w, acc)
            for first, at in ((4 * k, 4),) + (((64 + 4 * k, 28),) if k < 2 else ()):
                for t, a in enumerate((cs, hs, ss)):
                    to = at + 8 * t
                    here = (lane >= to) & (lane < to + 4)
                    acc = jnp.where(here, pltpu.roll(a, (to - first) % 128, 1), acc)
            out[k, rows, 512:640] = acc
        return 0

    lax.fori_loop(0, 8, body, 0)


def split(x):
    hi = x.astype(BF16)
    return hi, (x - hi.astype(F32)).astype(BF16)


def dot(a, b):
    return lax.dot_general(a, b, (((1,), (1,)), ((), ())), preferred_element_type=F32)


def place(g):
    return (g % 2) * 8 + g // 2


def corr_kernel(r, ah, al, eh, es, er, ce, co):
    volume = 1.0 / (ah.shape[1] * 256)
    lane = lane_of((64, 128))
    slot = (lane % 8 >= 4) & ((lane < 8) | ((lane >= 28) & (lane < 32)))

    def prepare(g, _):
        rows = pl.ds(pl.multiple_of(g * 64, 64), 64)
        to = pl.ds(pl.multiple_of(place(g) * 64, 64), 64)
        ah[to, :], al[to, :] = split(r[rows, :512])
        ext = r[rows, 512:640]
        zero = jnp.zeros_like(ext)
        chi, clo = [a.astype(F32) for a in split(jnp.where(slot, ext, zero))]
        er[to, :] = (chi + pltpu.roll(clo, 8, 1) + pltpu.roll(chi, 16, 1)).astype(BF16)
        for t, e in ((1, eh), (2, es)):
            hi, lo = [a.astype(F32) for a in split(jnp.where(slot, pltpu.roll(ext, 128 - 8 * t, 1), zero))]
            e[to, :] = (hi + pltpu.roll(hi, 8, 1) + pltpu.roll(lo, 16, 1)).astype(BF16)
        return 0

    lax.fori_loop(0, 16, prepare, 0)

    def corr(i, j):
        i, j = slice(i, i + 256), slice(j, j + 256)
        acc = dot(ah[i, :], ah[j, :]) + dot(ah[i, :], al[j, :]) + dot(al[i, :], ah[j, :])
        return acc * volume + dot(es[i, :], er[j, :])

    for q in range(2):
        for n, (i, j) in enumerate(((0, 0), (256, 0), (256, 256))):
            ce[q, n] = corr(q * 512 + i, q * 512 + j)
    for i in (0, 256):
        for j in (0, 256):
            co[i : i + 256, j : j + 256] = corr(512 + i, j)


def gram(which, ah, al, ph, lo, eh, er, ce, co, out, c):
    low = lane_of((64, 128)) < 64

    def ham(i, j):
        i, j = slice(i, i + 256), slice(j, j + 256)
        acc = dot(ph[i, :], ah[j, :]) + dot(ph[i, :], al[j, :]) + dot(lo[i, :], ah[j, :])
        acc += dot(ah[i, :], ph[j, :]) + dot(al[i, :], ph[j, :]) + dot(ah[i, :], lo[j, :])
        return acc + dot(eh[i, :], er[j, :])

    def tiles(e, f, t, get):
        for j in range(4):
            if f % 2:
                lower, upper = get(2 * j + 1, (f - 2 * j - 1) % 8 // 2), get(2 * j, (f - 2 * j - 1) % 8 // 2)
            else:
                lower, upper = get(2 * j, (f - 2 * j) % 8 // 2), get(2 * j + 1, (f - 2 * j - 2) % 8 // 2)
            out[e, t + j] = jnp.where(low, lower, upper)

    @pl.when(which == 0)
    def _():
        g = lax.broadcasted_iota(jnp.int32, (256, 256), 0) // 64
        h = lax.broadcasted_iota(jnp.int32, (256, 256), 1) // 64
        for q in range(2):
            at = q * 512
            c[q, :256, 256:] = ham(at, at + 256)
            c[q, 256:, :256] = ce[q, 1]
            c[q, :256, :256] = jnp.where(g <= h, ham(at, at), ce[q, 0])
            c[q, 256:, 256:] = jnp.where(g <= h, ham(at + 256, at + 256), ce[q, 2])
        for e in range(8):
            for q in range(2):
                tiles(e, (e - q) % 8, q * 4, lambda m, n: c[q, m * 64 : m * 64 + 64, n * 128 : n * 128 + 128])
            m = e // 2
            at = m * 64
            cols = slice(at // 128 * 128, at // 128 * 128 + 128)
            a, b = ce[e % 2, 0, at : at + 64, cols], ce[e % 2, 2, at : at + 64, cols]
            if m % 2:
                a = pltpu.roll(a, 64, 1)
            else:
                b = pltpu.roll(b, 64, 1)
            out[e, 8] = jnp.where(low, a, b)

    @pl.when(which == 1)
    def _():
        for i in (0, 256):
            for j in (0, 256):
                c[0, i : i + 256, j : j + 256] = ham(i, 512 + j)
        for e in range(8):
            tiles(e, e, 0, lambda m, n: c[0, m * 64 : m * 64 + 64, n * 128 : n * 128 + 128])
            tiles(e, e, 4, lambda m, n: co[m * 64 : m * 64 + 64, n * 128 : n * 128 + 128])
            out[e, 8] = jnp.zeros((64, 128), F32)


def send_kernel(ids, r, xh, pot, ah, al, eh, er, ce, co, out, ph, lo, c):
    volume = 1.0 / (ah.shape[1] * 256)
    lane = lane_of((64, 128))

    def prepare(g, _):
        rows = pl.ds(pl.multiple_of(g * 64, 64), 64)
        to = pl.ds(pl.multiple_of(place(g) * 64, 64), 64)
        ext = r[rows, 512:640]
        for x in range(4):
            cols = slice(x * 128, (x + 1) * 128)
            p = r[rows, cols]
            beside = r[rows, (x + 1) * 128 : (x + 2) * 128] if x < 3 else xh[rows, :]
            beside = beside + pltpu.roll(p, 120, 1)
            beside = beside + jnp.where(lane % 8 == 7, pltpu.roll(ext, 7 - x, 1), pltpu.roll(p, 127, 1))
            phi = (1.5 + 0.5 * pot[x : x + 1, :]) * p - 0.5 * beside
            ph[to, cols], lo[to, cols] = split(phi * volume)
        return 0

    lax.fori_loop(0, 16, prepare, 0)
    gram(1 - lax.rem(ids[1], 2), ah, al, ph, lo, eh, er, ce, co, out, c)


def keep_kernel(ids, ph, lo, ah, al, eh, er, ce, co, out, c):
    gram(lax.rem(ids[1], 2), ah, al, ph, lo, eh, er, ce, co, out, c)


def first_kernel(ids, keep, mate, s1, s2, s3, own):
    d = ids[1]
    north, x, h = lax.rem(d, 2) == 1, d // 4, lax.rem(d // 2, 2)

    def total(ref, i, across, along):
        e = jnp.where(north, along, across)
        ref[i] = keep[e] + mate[e]

    def part(dx, y):
        return lax.rem(x + dx, 4) * 2 + y

    for i in range(2):
        total(s1, i, part(1, i), part(i, 1 - h))
        total(s2, i, part(3, i), part(2 + i, 1 - h))
        total(own, i, part(0, i), part(i, h))
        total(own, 2 + i, part(0, i), part(2 + i, h))
        total(s3, i, part(2, i), part(2, i))


def second_kernel(ids, own, r1, r2, r3, keep, s1, s2, s3):
    d = ids[1]
    north, h = lax.rem(d, 2) == 1, lax.rem(d // 2, 2)

    @pl.when(jnp.logical_not(north))
    def _():
        def total(i):
            return own[i] + r1[i] + r2[i] + r3[i]

        keep[...] = total(h)
        s1[...] = total(1 - h)

    @pl.when(north)
    def _():
        keep[...] = own[0] + r1[0]
        s1[...] = own[1] + r1[1]
        s3[...] = own[2] + r2[0]
        s2[...] = own[3] + r2[1]


def rows_kernel(ids, keep, r1, r2, r3, out, total):
    d = ids[1]
    low = lane_of((64, 128)) < 64
    total[...] = keep[...] + r1[...]

    @pl.when(lax.rem(d, 2) == 1)
    def _():
        total[...] = total[...] + (r2[...] + r3[...])

    e = d // 2
    even = 1 - lax.rem(d, 2)

    def block(g, upper):
        m, p = g // 2, lax.rem(g, 2)
        t = total[p * 4 + m // 2]
        half = lax.rem(m + e + even * p, 2)
        return jnp.where(half == upper, t, pltpu.roll(t, 64, 1))

    for g in range(16):
        h = lax.rem(d - g + 16, 16)
        own = total[8] if g >= 8 else pltpu.roll(total[8], 64, 1)
        out[g] = jnp.where(low, block(jnp.int32(g), 0), jnp.where(h == g, own, block(h, 1)))


def finish_kernel(ids, parts, out):
    b, d = ids[0], ids[1]
    h = lax.rem(d - b + 16, 16)
    t = parts[0]
    for s in range(1, 16):
        t = t + parts[s]
    low = lane_of((64, 128)) < 64
    flipped = jnp.concatenate([t, t], axis=0).T[64:, :]
    upper = jnp.where(low, t, flipped)
    lower = jnp.where(low, flipped, pltpu.roll(t, 64, 1))
    left = jnp.where(lax.rem(d, 2) == 1, lax.rem(b, 2), (b > h).astype(jnp.int32)) == 0
    t = jnp.where(b == h, t, jnp.where(left, upper, lower))
    for i in range(16):
        out[i] = t


def assemble_kernel(ids, parts, ham, corr):
    b = ids[0]
    low = lane_of((64, 128)) < 64
    for j in range(8):
        t0 = parts[lax.rem(2 * j + b, 16)]
        t1 = parts[lax.rem(2 * j + 1 + b, 16)]
        cols = slice(j * 128, (j + 1) * 128)
        ham[:, cols] = jnp.where(low, t0, pltpu.roll(t1, 64, 1))
        corr[:, cols] = jnp.where(low, pltpu.roll(t0, 64, 1), t1)


def call(kernel, args, outs, scratch=(), flops=0, mib=8):
    specs = [SMEM if a.dtype == jnp.int32 else VMEM for a in args]
    size = sum(a.size * a.dtype.itemsize for a in (*args, *outs))
    single = len(outs) == 1
    return pl.pallas_call(
        kernel,
        out_shape=outs[0] if single else outs,
        in_specs=specs,
        out_specs=VMEM if single else [VMEM] * len(outs),
        scratch_shapes=scratch,
        compiler_params=pltpu.CompilerParams(vmem_limit_bytes=mib * 1024 * 1024),
        cost_estimate=pl.CostEstimate(flops=flops or 8 * size, bytes_accessed=size, transcendentals=0),
    )(*args)


def shape(*dims, dtype=F32):
    return jax.ShapeDtypeStruct(dims, dtype)


def rows_product(left, right):
    return lax.dot_general(left, right, (((1,), (1,)), ((), ())), precision=HI, preferred_element_type=F32)


def moves(south, north):
    pairs = []
    for d in range(16):
        x, h, c = d // 4, d // 2 % 2, d % 2
        step = north if c else south
        if step:
            pairs.append((d, (x + step[0]) % 4 * 4 + (h + step[1]) % 2 * 2 + c))
    return pairs


def reduced_over_dom(ids, keep, mate):
    piece = (9, 64, 128)
    sends = call(first_kernel, (ids, keep, mate), [shape(n, *piece) for n in (2, 2, 2, 4)], mib=16)
    steps = (((1, 0), (0, 1)), ((3, 0), (0, 1)), ((2, 0), None))
    got = [lax.ppermute(v, "dom", moves(*s)) for v, s in zip(sends, steps)]
    keep, *sends = call(second_kernel, (ids, sends[3], *got), [shape(*piece)] * 4, mib=12)
    steps = (((0, 1), (1, 0)), (None, (3, 0)), (None, (2, 0)))
    got = [lax.ppermute(v, "dom", moves(*s)) for v, s in zip(sends, steps)]
    return call(rows_kernel, (ids, keep, *got), (shape(16, 64, 128),), [pltpu.VMEM(piece, F32)], mib=8)


def on_device(wavefunctions, potential, projectors, hamiltonian_correction, delta_s, projector_count):
    bands, cx, ny, nz = wavefunctions.shape
    atoms, slots = hamiltonian_correction.shape[:2]
    b, d = lax.axis_index("band"), lax.axis_index("dom")
    ids = jnp.stack([b, d]).astype(jnp.int32)

    mask = (jnp.arange(slots, dtype=jnp.int32)[None, :] < projector_count[:, None]).astype(F32).reshape(-1)
    proj = projectors.reshape(atoms * slots, cx * ny * nz)
    coef = rows_product(wavefunctions.reshape(bands, cx * ny * nz), proj) * mask[None, :]
    coef = jnp.pad(coef, ((0, 0), (0, 128 - atoms * slots)))

    def coupled(m):
        m = 0.5 * (m + jnp.swapaxes(m, 1, 2))
        full = jnp.eye(atoms, dtype=F32)[:, None, :, None] * m[:, :, None, :]
        full = full.reshape(atoms * slots, atoms * slots)
        full = jnp.pad(full, (0, 128 - atoms * slots))
        return jnp.dot(coef, full, precision=HI, preferred_element_type=F32)

    wh, ws = coupled(hamiltonian_correction), coupled(delta_s)
    parts = call(spread_kernel, (wavefunctions.reshape(bands * cx * ny, nz), coef, wh, ws), (shape(16, bands, 640),))
    slab = lax.all_to_all(parts, "band", 0, 0, tiled=True).reshape(16 * bands, 640)
    ahead = lax.ppermute(slab[:, :128], "dom", [((i + 1) % 16, i) for i in range(16)])
    pot = lax.dynamic_slice_in_dim(potential, b * 8, 8, 2).reshape(cx, ny * 8)
    m = 16 * bands
    wide, ext = shape(m, 512, dtype=BF16), shape(m, 128, dtype=BF16)
    work = 2 * m * m * 512
    quads = [pltpu.VMEM((2, 512, 512), F32)]
    ah, al, eh, es, er, ce, co = call(
        corr_kernel, (slab,), [wide, wide, ext, ext, ext, shape(2, 3, 256, 256), shape(512, 512)], flops=3 * work, mib=12
    )
    corr = (ah, al, eh, er, ce, co)
    parts = shape(8, 9, 64, 128)
    send, ph, lo = call(send_kernel, (ids, slab, ahead, pot, *corr), [parts, wide, wide], quads, 3 * work, 20)
    mate = lax.ppermute(send, "dom", [(i, i ^ 1) for i in range(16)])
    keep = call(keep_kernel, (ids, ph, lo, *corr), [parts], quads, 3 * work, 18)
    parts = reduced_over_dom(ids, keep, mate)
    parts = lax.all_to_all(parts, "band", 0, 0, tiled=True)
    parts = call(finish_kernel, (ids, parts), (shape(16, 64, 128),))
    parts = lax.all_to_all(parts, "dom", 0, 0, tiled=True)
    return call(assemble_kernel, (ids, parts), (shape(64, 1024), shape(64, 1024)))


def solution(mesh):
    placed = (
        P("band", "dom", None, None),
        P("dom", None, None),
        P("dom", None, None, None, None),
        P("dom", None, None),
        P("dom", None, None),
        P("dom"),
    )
    return jax.shard_map(
        on_device,
        mesh=mesh,
        in_specs=placed,
        out_specs=(P("band", None), P("band", None)),
        check_vma=False,
    )
```

```python
import jax
import jax.numpy as jnp
from jax import lax
from jax.experimental import pallas as pl
from jax.experimental.pallas import tpu as pltpu
from jax.sharding import PartitionSpec as P

F32 = jnp.float32
BF16 = jnp.bfloat16
HI = lax.Precision.HIGHEST
VMEM = pl.BlockSpec(memory_space=pltpu.VMEM)
SMEM = pl.BlockSpec(memory_space=pltpu.SMEM)


def lane_of(shape):
    return lax.broadcasted_iota(jnp.int32, shape, len(shape) - 1)


def turn(x, n):
    n = n % 128
    return pltpu.roll(x, n, 1) if n else x


def spread_kernel(wf, out, held, ready, sems):
    lane = lane_of((8, 128))
    block = lane // 8

    def fetch(i):
        rows = pl.ds(pl.multiple_of(i * 512, 512), 512)
        return pltpu.make_async_copy(wf.at[rows], held.at[rows], sems.at[i])

    for i in range(8):
        fetch(i).start()

    def body(bg, _):
        fetch(bg).wait()
        for x in range(4):
            v = [held[pl.ds(bg * 512 + x * 16 + y, 8, stride=64), :] for y in range(16)]
            for s in (1, 2, 4, 8):
                low = (block & s) == 0
                nxt = list(v)
                for y in range(16):
                    if not y & s:
                        a, b = v[y], v[y + s]
                        nxt[y] = jnp.where(low, a, turn(b, s * 8))
                        nxt[y + s] = jnp.where(low, turn(a, -s * 8), b)
                v = nxt
            rows = pl.ds(pl.multiple_of(x * 64 + bg * 8, 8), 8)
            for k in range(16):
                ready[k, rows, :] = v[k]
        return 0

    lax.fori_loop(0, 8, body, 0)
    copy = pltpu.make_async_copy(ready, out, sems.at[8])
    copy.start()
    copy.wait()


def edge_kernel(r, first, below):
    lane = lane_of((32, 128))

    def body(g, _):
        first[g] = r[g, :64, :]
        acc = r[g, :32, :]
        for i in range(1, 8):
            at = i % 4 * 64 + i // 4 * 32
            acc = jnp.where(lane % 8 == i, turn(r[g, at : at + 32, :], i), acc)
        below[g] = acc
        return 0

    lax.fori_loop(0, 16, body, 0)


def split(x):
    hi = x.astype(BF16)
    return hi, (x - hi.astype(F32)).astype(BF16)


def dot(a, b):
    return lax.dot_general(a, b, (((1,), (1,)), ((), ())), preferred_element_type=F32)


def place(g):
    return (g % 2) * 8 + g // 2


FIRST = (0, 8, 10)


def couple_kernel(hc, ds, out):
    lane = lane_of((24, 128))
    out[...] = jnp.zeros_like(out)
    for t, m in enumerate((hc, ds)):
        for a in range(4):
            out[t, a, :16, :18] = m[a, :16, :]
            out[t, a, 16:, :18] = m[a, 10:18, :]
            v = out[t, a]
            out[t, a] = jnp.where(lane < 16, v, jnp.where(lane < 24, turn(v, 6), jnp.zeros_like(v)))


def coef_kernel(ids, count, wf, proj, sym, potential, pot, *refs):
    outs, (rows, padded) = refs[:16], refs[16:]
    for x in range(4):
        v = pltpu.roll(potential[x], lax.rem(128 - 8 * ids[0], 128), 1)
        own = lane_of((16, 128)) // 8 == lax.broadcasted_iota(jnp.int32, (16, 128), 0)
        v = jnp.where(own, pltpu.roll(v, 0, 1, stride=8, stride_axis=0), jnp.zeros_like(v))
        pot[x : x + 1, :] = jnp.sum(v, axis=0, keepdims=True)

    def add(xy, acc):
        p = [proj[pl.ds((18 * a + f) * 64 + xy, 8, stride=64), :] for a in range(4) for f in FIRST]
        ph, plo = split(jnp.concatenate(p, axis=0))
        wh, wlo = split(wf[pl.ds(xy, 64, stride=64), :])
        return acc + (dot(ph, wh) + dot(ph, wlo) + dot(plo, wh))

    acc = lax.fori_loop(0, 64, add, jnp.zeros((96, 64), F32))
    row = lax.broadcasted_iota(jnp.int32, (24, 64), 0)
    slot = jnp.where(row < 16, row, row - 6)
    rows[...] = jnp.zeros_like(rows)
    for a in range(4):
        kept = (slot < count[a]) & ((row < 16) | (slot >= 16))
        c = jnp.where(kept, acc[a * 24 : a * 24 + 24], jnp.zeros((24, 64), F32))
        padded[...] = jnp.zeros_like(padded)
        padded[:24, :] = c
        found = [c]
        for t in range(2):
            m = sym[t, a]
            right = jnp.dot(m, padded[...], precision=HI, preferred_element_type=F32)
            left = lax.dot_general(m, c, (((0,), (0,)), ((), ())), precision=HI, preferred_element_type=F32)
            found.append(0.5 * (right + left[:24]))
        for t, v in enumerate(found):
            for j in range(3):
                rows[a * 3 + j, t // 2 * 8 : t // 2 * 8 + 8, t % 2 * 64 : t % 2 * 64 + 64] = v[j * 8 : j * 8 + 8]
    for i, out in enumerate(outs):
        out[...] = rows[lax.rem(ids[0] + i, 16)]


def corr_kernel(ids, r, pot, *refs):
    came, (ah, al, part, eh, es, er, ce, co, cc) = refs[:16], refs[16:]
    volume = 1.0 / (ah.shape[1] * 256)
    lane = lane_of((64, 128))
    for i, v in enumerate(came):
        at = pl.ds(pl.multiple_of(lax.rem(ids[0] + 16 - i, 16) * 8, 8), 8)
        cc[0, at, :], cc[1, at, :] = v[:8, :], v[8:, :]
    two = cc[0].T
    slots = [two[:64], two[64:], cc[1].T[:64]]
    zero = jnp.zeros((64, 128), F32)

    def prepare(g, _):
        to = pl.ds(pl.multiple_of(place(g) * 64, 64), 64)
        for x in range(4):
            cols = slice(x * 128, (x + 1) * 128)
            p = r[g, x * 64 : (x + 1) * 64, :]
            ah[to, cols], al[to, cols] = split(p)
            beside = turn(p, -8) + jnp.where(lane % 8 == 7, zero, turn(p, -1))
            if x < 3:
                beside = beside + r[g, (x + 1) * 64 : (x + 2) * 64, :]
            part[to, cols] = (1.5 + 0.5 * pot[x : x + 1, :]) * p - 0.5 * beside
        back = lax.rem(128 - 8 * g, 128)
        for t, e in enumerate((er, eh, es)):
            hi, lo = [v.astype(F32) for v in split(jnp.where(lane < 8, pltpu.roll(slots[t], back, 1), zero))]
            second, third = (hi, lo) if t else (lo, hi)
            e[to, :] = (hi + turn(second, 8) + turn(third, 16)).astype(BF16)
        return 0

    lax.fori_loop(0, 16, prepare, 0)

    def corr(i, j):
        i, j = slice(i, i + 256), slice(j, j + 256)
        acc = dot(ah[i, :], ah[j, :]) + dot(ah[i, :], al[j, :]) + dot(al[i, :], ah[j, :])
        return acc * volume + dot(es[i, :], er[j, :])

    for q in range(2):
        for n, (i, j) in enumerate(((0, 0), (256, 0), (256, 256))):
            ce[q, n] = corr(q * 512 + i, q * 512 + j)
    for i in (0, 256):
        for j in (0, 256):
            co[i : i + 256, j : j + 256] = corr(512 + i, j)


def gram(which, ah, al, ph, lo, eh, er, ce, co, out, c):
    low = lane_of((64, 128)) < 64

    def ham(i, j):
        i, j = slice(i, i + 256), slice(j, j + 256)
        acc = dot(ph[i, :], ah[j, :]) + dot(ph[i, :], al[j, :]) + dot(lo[i, :], ah[j, :])
        acc += dot(ah[i, :], ph[j, :]) + dot(al[i, :], ph[j, :]) + dot(ah[i, :], lo[j, :])
        return acc + dot(eh[i, :], er[j, :])

    def tiles(e, f, t, get):
        for j in range(4):
            if f % 2:
                lower, upper = get(2 * j + 1, (f - 2 * j - 1) % 8 // 2), get(2 * j, (f - 2 * j - 1) % 8 // 2)
            else:
                lower, upper = get(2 * j, (f - 2 * j) % 8 // 2), get(2 * j + 1, (f - 2 * j - 2) % 8 // 2)
            out[e, t + j] = jnp.where(low, lower, upper)

    @pl.when(which == 0)
    def _():
        g = lax.broadcasted_iota(jnp.int32, (256, 256), 0) // 64
        h = lax.broadcasted_iota(jnp.int32, (256, 256), 1) // 64
        for q in range(2):
            at = q * 512
            c[q, :256, 256:] = ham(at, at + 256)
            c[q, 256:, :256] = ce[q, 1]
            c[q, :256, :256] = jnp.where(g <= h, ham(at, at), ce[q, 0])
            c[q, 256:, 256:] = jnp.where(g <= h, ham(at + 256, at + 256), ce[q, 2])
        for e in range(8):
            for q in range(2):
                tiles(e, (e - q) % 8, q * 4, lambda m, n: c[q, m * 64 : m * 64 + 64, n * 128 : n * 128 + 128])
            m = e // 2
            at = m * 64
            cols = slice(at // 128 * 128, at // 128 * 128 + 128)
            a, b = ce[e % 2, 0, at : at + 64, cols], ce[e % 2, 2, at : at + 64, cols]
            if m % 2:
                a = pltpu.roll(a, 64, 1)
            else:
                b = pltpu.roll(b, 64, 1)
            out[e, 8] = jnp.where(low, a, b)

    @pl.when(which == 1)
    def _():
        for i in (0, 256):
            for j in (0, 256):
                c[0, i : i + 256, j : j + 256] = ham(i, 512 + j)
        for e in range(8):
            tiles(e, e, 0, lambda m, n: c[0, m * 64 : m * 64 + 64, n * 128 : n * 128 + 128])
            tiles(e, e, 4, lambda m, n: co[m * 64 : m * 64 + 64, n * 128 : n * 128 + 128])
            out[e, 8] = jnp.zeros((64, 128), F32)


def send_kernel(ids, part, xh, zh, ah, al, eh, er, ce, co, out, ph, lo, c):
    volume = 1.0 / (ah.shape[1] * 256)
    lane = lane_of((64, 128))

    def prepare(g, _):
        to = pl.ds(pl.multiple_of(place(g) * 64, 64), 64)
        two = zh[g]
        ext = jnp.concatenate([two, turn(two, -4)], axis=0)
        for x in range(4):
            cols = slice(x * 128, (x + 1) * 128)
            beside = jnp.where(lane % 8 == 7, turn(ext, 7 - x), jnp.zeros((64, 128), F32))
            if x == 3:
                beside = beside + xh[g]
            ph[to, cols], lo[to, cols] = split((part[to, cols] - 0.5 * beside) * volume)
        return 0

    lax.fori_loop(0, 16, prepare, 0)
    gram(1 - lax.rem(ids[1], 2), ah, al, ph, lo, eh, er, ce, co, out, c)


def keep_kernel(ids, ph, lo, ah, al, eh, er, ce, co, out, c):
    gram(lax.rem(ids[1], 2), ah, al, ph, lo, eh, er, ce, co, out, c)


def first_kernel(ids, keep, mate, s1, s2, s3, own):
    d = ids[1]
    north, x, h = lax.rem(d, 2) == 1, d // 4, lax.rem(d // 2, 2)

    def total(ref, i, across, along):
        e = jnp.where(north, along, across)
        ref[i] = keep[e] + mate[e]

    def part(dx, y):
        return lax.rem(x + dx, 4) * 2 + y

    for i in range(2):
        total(s1, i, part(1, i), part(i, 1 - h))
        total(s2, i, part(3, i), part(2 + i, 1 - h))
        total(own, i, part(0, i), part(i, h))
        total(own, 2 + i, part(0, i), part(2 + i, h))
        total(s3, i, part(2, i), part(2, i))


def second_kernel(ids, own, r1, r2, r3, keep, s1, s2, s3):
    d = ids[1]
    north, h = lax.rem(d, 2) == 1, lax.rem(d // 2, 2)

    @pl.when(jnp.logical_not(north))
    def _():
        def total(i):
            return own[i] + r1[i] + r2[i] + r3[i]

        keep[...] = total(h)
        s1[...] = total(1 - h)

    @pl.when(north)
    def _():
        keep[...] = own[0] + r1[0]
        s1[...] = own[1] + r1[1]
        s3[...] = own[2] + r2[0]
        s2[...] = own[3] + r2[1]


def rows_kernel(ids, keep, r1, r2, r3, out, total):
    d = ids[1]
    low = lane_of((64, 128)) < 64
    total[...] = keep[...] + r1[...]

    @pl.when(lax.rem(d, 2) == 1)
    def _():
        total[...] = total[...] + (r2[...] + r3[...])

    e = d // 2
    even = 1 - lax.rem(d, 2)

    def block(g, upper):
        m, p = g // 2, lax.rem(g, 2)
        t = total[p * 4 + m // 2]
        half = lax.rem(m + e + even * p, 2)
        return jnp.where(half == upper, t, pltpu.roll(t, 64, 1))

    for g in range(16):
        h = lax.rem(d - g + 16, 16)
        own = total[8] if g >= 8 else pltpu.roll(total[8], 64, 1)
        out[g] = jnp.where(low, block(jnp.int32(g), 0), jnp.where(h == g, own, block(h, 1)))


def finish_kernel(ids, parts, out):
    b, d = ids[0], ids[1]
    h = lax.rem(d - b + 16, 16)
    t = parts[0]
    for s in range(1, 16):
        t = t + parts[s]
    low = lane_of((64, 128)) < 64
    flipped = jnp.concatenate([t, t], axis=0).T[64:, :]
    upper = jnp.where(low, t, flipped)
    lower = jnp.where(low, flipped, pltpu.roll(t, 64, 1))
    left = jnp.where(lax.rem(d, 2) == 1, lax.rem(b, 2), (b > h).astype(jnp.int32)) == 0
    t = jnp.where(b == h, t, jnp.where(left, upper, lower))
    out[...] = t


def join_kernel(a, b, c, d, out):
    for i, v in enumerate((a, b, c, d)):
        out[i] = v[...]


def assemble_kernel(ids, own, r1, r2, r3, ham, corr, parts):
    b, d = ids[0], ids[1]
    low = lane_of((64, 128)) < 64
    for i, v in enumerate((own, r1, r2, r3)):
        parts[4 * i : 4 * i + 4] = v[...]

    def piece(h):
        at = lax.rem(h + b, 16)
        ahead = lax.rem(at // 4 - d // 4 + 4, 4)
        return parts[ahead * 4 + (lax.rem(at, 4) ^ lax.rem(d, 4))]

    for j in range(8):
        t0, t1 = piece(2 * j), piece(2 * j + 1)
        cols = slice(j * 128, (j + 1) * 128)
        ham[:, cols] = jnp.where(low, t0, turn(t1, 64))
        corr[:, cols] = jnp.where(low, turn(t0, 64), t1)


def call(kernel, args, outs, scratch=(), flops=0, mib=8):
    specs = [SMEM if a.dtype == jnp.int32 else VMEM for a in args]
    size = sum(a.size * a.dtype.itemsize for a in (*args, *outs))
    single = len(outs) == 1
    return pl.pallas_call(
        kernel,
        out_shape=outs[0] if single else outs,
        in_specs=specs,
        out_specs=VMEM if single else [VMEM] * len(outs),
        scratch_shapes=scratch,
        compiler_params=pltpu.CompilerParams(vmem_limit_bytes=mib * 1024 * 1024),
        cost_estimate=pl.CostEstimate(flops=flops or 8 * size, bytes_accessed=size, transcendentals=0),
    )(*args)


def shape(*dims, dtype=F32):
    return jax.ShapeDtypeStruct(dims, dtype)


def moves(south, north):
    pairs = []
    for d in range(16):
        x, h, c = d // 4, d // 2 % 2, d % 2
        step = north if c else south
        if step:
            pairs.append((d, (x + step[0]) % 4 * 4 + (h + step[1]) % 2 * 2 + c))
    return pairs


def reduced_over_dom(ids, keep, mate):
    piece = (9, 64, 128)
    sends = call(first_kernel, (ids, keep, mate), [shape(n, *piece) for n in (2, 2, 2, 4)], mib=16)
    steps = (((1, 0), (0, 1)), ((3, 0), (0, 1)), ((2, 0), None))
    got = [lax.ppermute(v, "dom", moves(*s)) for v, s in zip(sends, steps)]
    keep, *sends = call(second_kernel, (ids, sends[3], *got), [shape(*piece)] * 4, mib=12)
    steps = (((0, 1), (1, 0)), (None, (3, 0)), (None, (2, 0)))
    got = [lax.ppermute(v, "dom", moves(*s)) for v, s in zip(sends, steps)]
    return call(rows_kernel, (ids, keep, *got), (shape(16, 64, 128),), [pltpu.VMEM(piece, F32)], mib=8)


def on_device(wavefunctions, potential, projectors, hamiltonian_correction, delta_s, projector_count):
    bands, cx, ny, nz = wavefunctions.shape
    atoms, slots = hamiltonian_correction.shape[:2]
    b, d = lax.axis_index("band"), lax.axis_index("dom")
    ids = jnp.stack([b, d]).astype(jnp.int32)

    flat = cx * ny
    wf = wavefunctions.reshape(bands * flat, nz)
    parts = pl.pallas_call(
        spread_kernel,
        out_shape=shape(16, cx * bands, 128),
        in_specs=[pl.BlockSpec(memory_space=pltpu.HBM)],
        out_specs=pl.BlockSpec(memory_space=pltpu.HBM),
        scratch_shapes=[
            pltpu.VMEM((bands * flat, nz), F32),
            pltpu.VMEM((16, cx * bands, 128), F32),
            pltpu.SemaphoreType.DMA((9,)),
        ],
        compiler_params=pltpu.CompilerParams(vmem_limit_bytes=61 * 1024 * 1024),
    )(wf)
    slab = lax.all_to_all(parts, "band", 0, 0, tiled=True)

    proj = projectors.reshape(atoms * slots * flat, nz)
    wf, proj, potential, hamiltonian_correction, delta_s, parts = lax.optimization_barrier(
        (wf, proj, potential, hamiltonian_correction, delta_s, parts)
    )
    sym = call(couple_kernel, (hamiltonian_correction, delta_s), (shape(2, atoms, 24, 128),), mib=2)
    pot, *cc = call(
        coef_kernel,
        (ids, projector_count, wf, proj, sym, potential),
        [shape(cx, nz)] + [shape(16, 128)] * 16,
        [pltpu.VMEM((16, 16, 128), F32), pltpu.VMEM((128, bands), F32)],
    )
    cc = [lax.ppermute(v, "band", [(j, (j + i) % 16) for j in range(16)]) if i else v for i, v in enumerate(cc)]
    slab, pot, *cc = lax.optimization_barrier((slab, pot, *cc))
    first, below = call(edge_kernel, (slab,), [shape(16, bands, 128), shape(16, bands // 2, 128)], mib=6)
    back = [((i + 1) % 16, i) for i in range(16)]
    ahead, above = lax.ppermute(first, "dom", back), lax.ppermute(below, "band", back)
    m = 16 * bands
    wide, ext = shape(m, 512, dtype=BF16), shape(m, 128, dtype=BF16)
    work = 2 * m * m * 512
    quads = [pltpu.VMEM((2, 512, 512), F32)]
    ah, al, part, eh, es, er, ce, co = call(
        corr_kernel,
        (ids, slab, pot, *cc),
        [wide, wide, shape(m, 512), ext, ext, ext, shape(2, 3, 256, 256), shape(512, 512)],
        [pltpu.VMEM((2, 128, 128), F32)],
        3 * work,
        16,
    )
    corr = (ah, al, eh, er, ce, co)
    parts = shape(8, 9, 64, 128)
    send, ph, lo = call(send_kernel, (ids, part, ahead, above, *corr), [parts, wide, wide], quads, 3 * work, 20)
    mate = lax.ppermute(send, "dom", [(i, i ^ 1) for i in range(16)])
    keep = call(keep_kernel, (ids, ph, lo, *corr), [parts], quads, 3 * work, 18)
    parts = reduced_over_dom(ids, keep, mate)
    parts = lax.all_to_all(parts, "band", 0, 0, tiled=True)
    own = call(finish_kernel, (ids, parts), (shape(64, 128),))
    near = [lax.ppermute(own, "dom", [(i, i ^ j) for i in range(16)]) for j in (1, 2, 3)]
    own = call(join_kernel, (own, *near), (shape(4, 64, 128),))
    far = [lax.ppermute(own, "dom", [((i + 4 * j) % 16, i) for i in range(16)]) for j in (1, 2, 3)]
    return call(
        assemble_kernel,
        (ids, own, *far),
        (shape(64, 1024), shape(64, 1024)),
        [pltpu.VMEM((16, 64, 128), F32)],
    )


def solution(mesh):
    placed = (
        P("band", "dom", None, None),
        P("dom", None, None),
        P("dom", None, None, None, None),
        P("dom", None, None),
        P("dom", None, None),
        P("dom"),
    )
    return jax.shard_map(
        on_device,
        mesh=mesh,
        in_specs=placed,
        out_specs=(P("band", None), P("band", None)),
        check_vma=False,
    )
```

```python
import jax
import jax.numpy as jnp
from jax import lax
from jax.experimental import pallas as pl
from jax.experimental.pallas import tpu as pltpu
from jax.sharding import PartitionSpec as P

F32 = jnp.float32
BF16 = jnp.bfloat16
HI = lax.Precision.HIGHEST
VMEM = pl.BlockSpec(memory_space=pltpu.VMEM)
SMEM = pl.BlockSpec(memory_space=pltpu.SMEM)


def lane_of(shape):
    return lax.broadcasted_iota(jnp.int32, shape, len(shape) - 1)


def turn(x, n):
    n = n % 128
    return pltpu.roll(x, n, 1) if n else x


def spread_kernel(wf, out, held, ready, sems):
    lane = lane_of((8, 128))
    block = lane // 8

    def fetch(i):
        rows = pl.ds(pl.multiple_of(i * 512, 512), 512)
        return pltpu.make_async_copy(wf.at[rows], held.at[rows], sems.at[i])

    for i in range(8):
        fetch(i).start()

    def body(bg, _):
        fetch(bg).wait()
        for x in range(4):
            v = [held[pl.ds(bg * 512 + x * 16 + y, 8, stride=64), :] for y in range(16)]
            for s in (1, 2, 4, 8):
                low = (block & s) == 0
                nxt = list(v)
                for y in range(16):
                    if not y & s:
                        a, b = v[y], v[y + s]
                        nxt[y] = jnp.where(low, a, turn(b, s * 8))
                        nxt[y + s] = jnp.where(low, turn(a, -s * 8), b)
                v = nxt
            rows = pl.ds(pl.multiple_of(x * 64 + bg * 8, 8), 8)
            for k in range(16):
                ready[k, rows, :] = v[k]
        return 0

    lax.fori_loop(0, 8, body, 0)
    copy = pltpu.make_async_copy(ready, out, sems.at[8])
    copy.start()
    copy.wait()


def edge_kernel(r, below):
    lane = lane_of((32, 128))

    def body(g, _):
        acc = r[g, :32, :]
        for i in range(1, 8):
            at = i % 4 * 64 + i // 4 * 32
            acc = jnp.where(lane % 8 == i, turn(r[g, at : at + 32, :], i), acc)
        below[g] = acc
        return 0

    lax.fori_loop(0, 16, body, 0)


def split(x):
    hi = x.astype(BF16)
    return hi, (x - hi.astype(F32)).astype(BF16)


def dot(a, b):
    return lax.dot_general(a, b, (((1,), (1,)), ((), ())), preferred_element_type=F32)


def slots(e, er, i, j):
    return lax.dot_general(e[:, i], er[:, j], (((0,), (0,)), ((), ())), preferred_element_type=F32)


def place(g):
    return (g % 2) * 8 + g // 2


FIRST = (0, 8, 10)


def couple_kernel(hc, ds, out):
    lane = lane_of((24, 128))
    out[...] = jnp.zeros_like(out)
    for t, m in enumerate((hc, ds)):
        for a in range(4):
            out[t, a, :16, :18] = m[a, :16, :]
            out[t, a, 16:, :18] = m[a, 10:18, :]
            v = out[t, a]
            out[t, a] = jnp.where(lane < 16, v, jnp.where(lane < 24, turn(v, 6), jnp.zeros_like(v)))


def coef_kernel(ids, count, wf, proj, sym, potential, pot, *refs):
    outs, (rows, padded) = refs[:16], refs[16:]
    for x in range(4):
        v = pltpu.roll(potential[x], lax.rem(128 - 8 * ids[0], 128), 1)
        own = lane_of((16, 128)) // 8 == lax.broadcasted_iota(jnp.int32, (16, 128), 0)
        v = jnp.where(own, pltpu.roll(v, 0, 1, stride=8, stride_axis=0), jnp.zeros_like(v))
        pot[x : x + 1, :] = jnp.sum(v, axis=0, keepdims=True)

    def add(i, acc):
        p, w = [], []
        for xy in (4 * i, 4 * i + 1, 4 * i + 2, 4 * i + 3):
            p.append(jnp.concatenate([proj[pl.ds((18 * a + f) * 64 + xy, 8, stride=64), :] for a in range(4) for f in FIRST], axis=0))
            w.append(wf[pl.ds(xy, 64, stride=64), :])
        ph, plo = split(jnp.concatenate(p, axis=1))
        wh, wlo = split(jnp.concatenate(w, axis=1))
        return acc + (dot(ph, wh) + dot(ph, wlo) + dot(plo, wh))

    acc = lax.fori_loop(0, 16, add, jnp.zeros((96, 64), F32))
    row = lax.broadcasted_iota(jnp.int32, (24, 64), 0)
    slot = jnp.where(row < 16, row, row - 6)
    rows[...] = jnp.zeros_like(rows)
    for a in range(4):
        kept = (slot < count[a]) & ((row < 16) | (slot >= 16))
        c = jnp.where(kept, acc[a * 24 : a * 24 + 24], jnp.zeros((24, 64), F32))
        padded[...] = jnp.zeros_like(padded)
        padded[:24, :] = c
        found = [c]
        for t in range(2):
            m = sym[t, a]
            right = jnp.dot(m, padded[...], precision=HI, preferred_element_type=F32)
            left = lax.dot_general(m, c, (((0,), (0,)), ((), ())), precision=HI, preferred_element_type=F32)
            found.append(0.5 * (right + left[:24]))
        for t, v in enumerate(found):
            for j in range(3):
                rows[a * 3 + j, t // 2 * 8 : t // 2 * 8 + 8, t % 2 * 64 : t % 2 * 64 + 64] = v[j * 8 : j * 8 + 8]
    for i, out in enumerate(outs):
        out[...] = rows[lax.rem(ids[0] + i, 16)]


def corr_kernel(ids, r, pot, *refs):
    came, (ah, al, part, eh, es, er, ce, co, cc) = refs[:16], refs[16:]
    volume = 1.0 / (ah.shape[1] * 256)
    lane = lane_of((64, 128))
    for i, v in enumerate(came):
        cc[lax.rem(ids[0] + 16 - i, 16)] = v[...]
    half = lane_of((16, 128)) < 64
    none = jnp.zeros((8, 128), F32)
    for n in range(8):
        a, b = cc[4 * n % 16 + n // 4], cc[(4 * n + 2) % 16 + n // 4]
        x, y = jnp.where(half, a, turn(b, 64)), jnp.where(half, turn(a, 64), b)
        for t, (e, v) in enumerate(((er, x[:8]), (eh, y[:8]), (es, x[8:]))):
            hi, mid = [w.astype(F32) for w in split(v)]
            terms = [hi, hi, mid, none] if t else [hi, mid, hi, none]
            e[:, n * 128 : n * 128 + 128] = jnp.concatenate(terms, axis=0).astype(BF16)
    zero = jnp.zeros((64, 128), F32)

    def prepare(g, _):
        to = pl.ds(pl.multiple_of(place(g) * 64, 64), 64)
        for x in range(4):
            cols = slice(x * 128, (x + 1) * 128)
            p = r[g, x * 64 : (x + 1) * 64, :]
            ah[to, cols], al[to, cols] = split(p)
            beside = turn(p, -8) + jnp.where(lane % 8 == 7, zero, turn(p, -1))
            if x < 3:
                beside = beside + r[g, (x + 1) * 64 : (x + 2) * 64, :]
            part[to, cols] = (1.5 + 0.5 * pot[x : x + 1, :]) * p - 0.5 * beside
        return 0

    lax.fori_loop(0, 16, prepare, 0)

    def corr(i, j):
        i, j = slice(i, i + 256), slice(j, j + 256)
        acc = dot(ah[i, :], ah[j, :]) + dot(ah[i, :], al[j, :]) + dot(al[i, :], ah[j, :])
        return acc * volume + slots(es, er, i, j)

    for q in range(2):
        for n, (i, j) in enumerate(((0, 0), (256, 0), (256, 256))):
            ce[q, n] = corr(q * 512 + i, q * 512 + j)
    for i in (0, 256):
        for j in (0, 256):
            co[i : i + 256, j : j + 256] = corr(512 + i, j)


def gram(which, ah, al, ph, lo, eh, er, ce, co, out, c, on):
    low = lane_of((64, 128)) < 64

    def ham(i, j):
        i, j = slice(i, i + 256), slice(j, j + 256)
        acc = dot(ph[i, :], ah[j, :]) + dot(ph[i, :], al[j, :]) + dot(lo[i, :], ah[j, :])
        acc += dot(ah[i, :], ph[j, :]) + dot(al[i, :], ph[j, :]) + dot(ah[i, :], lo[j, :])
        return acc + slots(eh, er, i, j)

    def tiles(e, f, t, get):
        for j in range(4):
            if f % 2:
                lower, upper = get(2 * j + 1, (f - 2 * j - 1) % 8 // 2), get(2 * j, (f - 2 * j - 1) % 8 // 2)
            else:
                lower, upper = get(2 * j, (f - 2 * j) % 8 // 2), get(2 * j + 1, (f - 2 * j - 2) % 8 // 2)
            out[e, (t + j) * 64 : (t + j) * 64 + 64, :] = jnp.where(low, lower, upper)

    @pl.when(which == 0)
    def _():
        row = lax.broadcasted_iota(jnp.int32, (256, 256), 0)
        col = lax.broadcasted_iota(jnp.int32, (256, 256), 1)
        for q in range(2):
            at = q * 512
            c[q, :256, 256:] = ham(at, at + 256)
            c[q, 256:, :256] = ce[q, 1]
            for n in range(2):
                here, own = slice(n * 256, n * 256 + 256), ce[q, 2 * n]
                c[q, here, here] = jnp.where(row <= col, ham(at + n * 256, at + n * 256), own)
                diagonal = jnp.sum(jnp.where(row == col, own, jnp.zeros_like(own)), axis=0, keepdims=True)
                on[q, n] = jnp.broadcast_to(diagonal, (8, 256))
        for e in range(8):
            for q in range(2):
                tiles(e, (e - q) % 8, q * 4, lambda m, n: c[q, m * 64 : m * 64 + 64, n * 128 : n * 128 + 128])
            m = e // 2
            cols = slice(m // 2 * 128, m // 2 * 128 + 128)
            a, b = on[e % 2, 0, :, cols], on[e % 2, 1, :, cols]
            if m % 2:
                a = turn(a, 64)
            else:
                b = turn(b, 64)
            out[e, 512:, :] = jnp.where(low[:8], a, b)

    @pl.when(which == 1)
    def _():
        for i in (0, 256):
            for j in (0, 256):
                c[0, i : i + 256, j : j + 256] = ham(i, 512 + j)
        for e in range(8):
            tiles(e, e, 0, lambda m, n: c[0, m * 64 : m * 64 + 64, n * 128 : n * 128 + 128])
            tiles(e, e, 4, lambda m, n: co[m * 64 : m * 64 + 64, n * 128 : n * 128 + 128])
            out[e, 512:, :] = jnp.zeros((8, 128), F32)


def send_kernel(ids, part, xh, zh, ah, al, eh, er, ce, co, out, ph, lo, c, on):
    volume = 1.0 / (ah.shape[1] * 256)
    lane = lane_of((64, 128))

    def prepare(g, _):
        to = pl.ds(pl.multiple_of(place(g) * 64, 64), 64)
        two = zh[g]
        ext = jnp.concatenate([two, turn(two, -4)], axis=0)
        for x in range(4):
            cols = slice(x * 128, (x + 1) * 128)
            beside = jnp.where(lane % 8 == 7, turn(ext, 7 - x), jnp.zeros((64, 128), F32))
            if x == 3:
                beside = beside + xh[g]
            ph[to, cols], lo[to, cols] = split((part[to, cols] - 0.5 * beside) * volume)
        return 0

    lax.fori_loop(0, 16, prepare, 0)
    gram(1 - lax.rem(ids[1], 2), ah, al, ph, lo, eh, er, ce, co, out, c, on)


def keep_kernel(ids, ph, lo, ah, al, eh, er, ce, co, out, c, on):
    gram(lax.rem(ids[1], 2), ah, al, ph, lo, eh, er, ce, co, out, c, on)


def first_kernel(ids, keep, mate, s1, s2, s3, own):
    d = ids[1]
    north, x, h = lax.rem(d, 2) == 1, d // 4, lax.rem(d // 2, 2)

    def total(ref, i, across, along):
        e = jnp.where(north, along, across)
        ref[i] = keep[e] + mate[e]

    def part(dx, y):
        return lax.rem(x + dx, 4) * 2 + y

    for i in range(2):
        total(s1, i, part(1, i), part(i, 1 - h))
        total(s2, i, part(3, i), part(2 + i, 1 - h))
        total(own, i, part(0, i), part(i, h))
        total(own, 2 + i, part(0, i), part(2 + i, h))
        total(s3, i, part(2, i), part(2, i))


def second_kernel(ids, own, r1, r2, r3, keep, s1, s2, s3):
    d = ids[1]
    north, h = lax.rem(d, 2) == 1, lax.rem(d // 2, 2)

    @pl.when(jnp.logical_not(north))
    def _():
        def total(i):
            return own[i] + r1[i] + r2[i] + r3[i]

        keep[...] = total(h)
        s1[...] = total(1 - h)

    @pl.when(north)
    def _():
        keep[...] = own[0] + r1[0]
        s1[...] = own[1] + r1[1]
        s3[...] = own[2] + r2[0]
        s2[...] = own[3] + r2[1]


def rows_kernel(ids, keep, r1, r2, r3, out, total):
    d = ids[1]
    low = lane_of((64, 128)) < 64
    total[...] = keep[...] + r1[...]

    @pl.when(lax.rem(d, 2) == 1)
    def _():
        total[...] = total[...] + (r2[...] + r3[...])

    e = d // 2
    even = 1 - lax.rem(d, 2)

    def block(g, upper):
        m, p = g // 2, lax.rem(g, 2)
        t = total[pl.ds(pl.multiple_of((p * 4 + m // 2) * 64, 64), 64), :]
        half = lax.rem(m + e + even * p, 2)
        return jnp.where(half == upper, t, pltpu.roll(t, 64, 1))

    for g in range(16):
        h = lax.rem(d - g + 16, 16)
        own = jnp.broadcast_to(total[512:513, :], (64, 128))
        own = own if g >= 8 else turn(own, 64)
        out[g] = jnp.where(low, block(jnp.int32(g), 0), jnp.where(h == g, own, block(h, 1)))


def finish_kernel(ids, parts, out):
    b, d = ids[0], ids[1]
    h = lax.rem(d - b + 16, 16)
    t = parts[0]
    for s in range(1, 16):
        t = t + parts[s]
    low = lane_of((64, 128)) < 64
    both = jnp.concatenate([t, t], axis=0).T
    left, right, other = both[:64], both[64:], turn(t, 64)
    upper = jnp.where(low, t, right)
    lower = jnp.where(low, right, other)
    row, col = lax.broadcasted_iota(jnp.int32, (64, 128), 0), lane_of((64, 128)) % 64
    own = jnp.where(low, jnp.where(row <= col, t, left), jnp.where(row > col, other, jnp.where(row < col, left, t)))
    first = jnp.where(lax.rem(d, 2) == 1, lax.rem(b, 2), (b > h).astype(jnp.int32)) == 0
    out[...] = jnp.where(b == h, own, jnp.where(first, upper, lower))


def join_kernel(a, b, c, d, out):
    for i, v in enumerate((a, b, c, d)):
        out[i] = v[...]


def assemble_kernel(ids, own, r1, r2, r3, ham, corr, parts):
    b, d = ids[0], ids[1]
    low = lane_of((64, 128)) < 64
    for i, v in enumerate((own, r1, r2, r3)):
        parts[4 * i : 4 * i + 4] = v[...]

    def piece(h):
        at = lax.rem(h + b, 16)
        ahead = lax.rem(at // 4 - d // 4 + 4, 4)
        return parts[ahead * 4 + (lax.rem(at, 4) ^ lax.rem(d, 4))]

    for j in range(8):
        t0, t1 = piece(2 * j), piece(2 * j + 1)
        cols = slice(j * 128, (j + 1) * 128)
        ham[:, cols] = jnp.where(low, t0, turn(t1, 64))
        corr[:, cols] = jnp.where(low, turn(t0, 64), t1)


def call(kernel, args, outs, scratch=(), flops=0, mib=8):
    specs = [SMEM if a.dtype == jnp.int32 else VMEM for a in args]
    size = sum(a.size * a.dtype.itemsize for a in (*args, *outs))
    single = len(outs) == 1
    return pl.pallas_call(
        kernel,
        out_shape=outs[0] if single else outs,
        in_specs=specs,
        out_specs=VMEM if single else [VMEM] * len(outs),
        scratch_shapes=scratch,
        compiler_params=pltpu.CompilerParams(vmem_limit_bytes=mib * 1024 * 1024),
        cost_estimate=pl.CostEstimate(flops=flops or 8 * size, bytes_accessed=size, transcendentals=0),
    )(*args)


def shape(*dims, dtype=F32):
    return jax.ShapeDtypeStruct(dims, dtype)


def moves(south, north):
    pairs = []
    for d in range(16):
        x, h, c = d // 4, d // 2 % 2, d % 2
        step = north if c else south
        if step:
            pairs.append((d, (x + step[0]) % 4 * 4 + (h + step[1]) % 2 * 2 + c))
    return pairs


def reduced_over_dom(ids, keep, mate):
    piece = (520, 128)
    sends = call(first_kernel, (ids, keep, mate), [shape(n, *piece) for n in (2, 2, 2, 4)], mib=16)
    steps = (((1, 0), (0, 1)), ((3, 0), (0, 1)), ((2, 0), None))
    got = [lax.ppermute(v, "dom", moves(*s)) for v, s in zip(sends, steps)]
    keep, *sends = call(second_kernel, (ids, sends[3], *got), [shape(*piece)] * 4, mib=12)
    steps = (((0, 1), (1, 0)), (None, (3, 0)), (None, (2, 0)))
    got = [lax.ppermute(v, "dom", moves(*s)) for v, s in zip(sends, steps)]
    return call(rows_kernel, (ids, keep, *got), (shape(16, 64, 128),), [pltpu.VMEM(piece, F32)], mib=8)


def on_device(wavefunctions, potential, projectors, hamiltonian_correction, delta_s, projector_count):
    bands, cx, ny, nz = wavefunctions.shape
    atoms, slots = hamiltonian_correction.shape[:2]
    b, d = lax.axis_index("band"), lax.axis_index("dom")
    ids = jnp.stack([b, d]).astype(jnp.int32)

    flat = cx * ny
    wf = wavefunctions.reshape(bands * flat, nz)
    parts = pl.pallas_call(
        spread_kernel,
        out_shape=shape(16, cx * bands, 128),
        in_specs=[pl.BlockSpec(memory_space=pltpu.HBM)],
        out_specs=pl.BlockSpec(memory_space=pltpu.HBM),
        scratch_shapes=[
            pltpu.VMEM((bands * flat, nz), F32),
            pltpu.VMEM((16, cx * bands, 128), F32),
            pltpu.SemaphoreType.DMA((9,)),
        ],
        compiler_params=pltpu.CompilerParams(vmem_limit_bytes=61 * 1024 * 1024),
    )(wf)
    slab = lax.all_to_all(parts, "band", 0, 0, tiled=True)

    proj = projectors.reshape(atoms * slots * flat, nz)
    wf, proj, potential, hamiltonian_correction, delta_s, parts = lax.optimization_barrier(
        (wf, proj, potential, hamiltonian_correction, delta_s, parts)
    )
    sym = call(couple_kernel, (hamiltonian_correction, delta_s), (shape(2, atoms, 24, 128),), mib=2)
    pot, *cc = call(
        coef_kernel,
        (ids, projector_count, wf, proj, sym, potential),
        [shape(cx, nz)] + [shape(16, 128)] * 16,
        [pltpu.VMEM((16, 16, 128), F32), pltpu.VMEM((128, bands), F32)],
    )
    cc = [lax.ppermute(v, "band", [(j, (j + i) % 16) for j in range(16)]) if i else v for i, v in enumerate(cc)]
    slab, pot, *cc = lax.optimization_barrier((slab, pot, *cc))
    back = [((i + 1) % 16, i) for i in range(16)]
    ahead = lax.ppermute(slab[:, :bands], "dom", back)
    above = lax.ppermute(call(edge_kernel, (slab,), [shape(16, bands // 2, 128)], mib=4), "band", back)
    m = 16 * bands
    wide, ext = shape(m, 512, dtype=BF16), shape(32, m, dtype=BF16)
    work = 2 * m * m * 512
    quads = [pltpu.VMEM((2, 512, 512), F32), pltpu.VMEM((2, 2, 8, 256), F32)]
    ah, al, part, eh, es, er, ce, co = call(
        corr_kernel,
        (ids, slab, pot, *cc),
        [wide, wide, shape(m, 512), ext, ext, ext, shape(2, 3, 256, 256), shape(512, 512)],
        [pltpu.VMEM((16, 16, 128), F32)],
        3 * work,
        16,
    )
    corr = (ah, al, eh, er, ce, co)
    parts = shape(8, 520, 128)
    send, ph, lo = call(send_kernel, (ids, part, ahead, above, *corr), [parts, wide, wide], quads, 3 * work, 20)
    mate = lax.ppermute(send, "dom", [(i, i ^ 1) for i in range(16)])
    keep = call(keep_kernel, (ids, ph, lo, *corr), [parts], quads, 3 * work, 18)
    parts = reduced_over_dom(ids, keep, mate)
    parts = lax.all_to_all(parts, "band", 0, 0, tiled=True)
    own = call(finish_kernel, (ids, parts), (shape(64, 128),))
    near = [lax.ppermute(own, "dom", [(i, i ^ j) for i in range(16)]) for j in (1, 2, 3)]
    own = call(join_kernel, (own, *near), (shape(4, 64, 128),))
    far = [lax.ppermute(own, "dom", [((i + 4 * j) % 16, i) for i in range(16)]) for j in (1, 2, 3)]
    return call(
        assemble_kernel,
        (ids, own, *far),
        (shape(64, 1024), shape(64, 1024)),
        [pltpu.VMEM((16, 64, 128), F32)],
    )


def solution(mesh):
    placed = (
        P("band", "dom", None, None),
        P("dom", None, None),
        P("dom", None, None, None, None),
        P("dom", None, None),
        P("dom", None, None),
        P("dom"),
    )
    return jax.shard_map(
        on_device,
        mesh=mesh,
        in_specs=placed,
        out_specs=(P("band", None), P("band", None)),
        check_vma=False,
    )
```

```python
import jax
import jax.numpy as jnp
from jax import lax
from jax.experimental import pallas as pl
from jax.experimental.pallas import tpu as pltpu
from jax.sharding import PartitionSpec as P


F32 = jnp.float32
BF16 = jnp.bfloat16
HI = lax.Precision.HIGHEST
VMEM = pl.BlockSpec(memory_space=pltpu.VMEM)
SMEM = pl.BlockSpec(memory_space=pltpu.SMEM)


def lane_of(shape):
    return lax.broadcasted_iota(jnp.int32, shape, len(shape) - 1)


def turn(x, n):
    n = n % 128
    return pltpu.roll(x, n, 1) if n else x


MOVES = [(0, 0)] + [(y, z) for z in (4, 3, -3, 2, -2, 1, -1) for y in (0, 1)] + [(1, 0)]


def band_at(b, move, sign=1):
    return (b // 8 + move[0]) % 2 * 8 + (b + sign * move[1] + 8) % 8


def spread_kernel(wf, out, last, held, ready, sems):
    lane = lane_of((8, 128))
    block = lane // 8

    def fetch(i):
        rows = pl.ds(pl.multiple_of(i * 512, 512), 512)
        return pltpu.make_async_copy(wf.at[rows], held.at[rows], sems.at[i])

    for i in range(8):
        fetch(i).start()

    def body(bg, _):
        fetch(bg).wait()
        for x in range(4):
            v = [held[pl.ds(bg * 512 + x * 16 + y, 8, stride=64), :] for y in range(16)]
            for s in (1, 2, 4, 8):
                low = (block & s) == 0
                nxt = list(v)
                for y in range(16):
                    if not y & s:
                        a, b = v[y], v[y + s]
                        if s == 8:
                            a_high = b_low = turn(jnp.where(low, b, a), 64)
                        else:
                            b_low, a_high = turn(b, s * 8), turn(a, -s * 8)
                        nxt[y] = jnp.where(low, a, b_low)
                        nxt[y + s] = jnp.where(low, a_high, b)
                v = nxt
            rows = pl.ds(pl.multiple_of(x * 64 + bg * 8, 8), 8)
            for k in range(16):
                ready[k, rows, :] = v[k]
        return 0

    lax.fori_loop(0, 8, body, 0)
    one = pltpu.make_async_copy(ready.at[:, :192], out, sems.at[8])
    two = pltpu.make_async_copy(ready.at[:, 192:], last, sems.at[9])
    one.start()
    two.start()
    one.wait()
    two.wait()


def edge_kernel(r, first, below):
    lane = lane_of((32, 128))

    def body(g, _):
        first[g] = r[g, :64, :]
        acc = r[g, :32, :]
        for i in (1, 2, 4, 5, 6):
            at = i % 4 * 64 + i // 4 * 32
            acc = jnp.where(lane % 8 == i, turn(r[g, at : at + 32, :], i), acc)
        below[g] = acc
        return 0

    lax.fori_loop(0, 16, body, 0)


def split(x):
    hi = x.astype(BF16)
    return hi, (x - hi.astype(F32)).astype(BF16)


def dot(a, b):
    return lax.dot_general(a, b, (((1,), (1,)), ((), ())), preferred_element_type=F32)


def slots(e, er, i, j):
    return lax.dot_general(e[:, i], er[:, j], (((0,), (0,)), ((), ())), preferred_element_type=F32)


def place(g):
    return (g % 2) * 8 + g // 2


FIRST = (0, 8, 10)


def couple_kernel(hc, ds, out):
    lane = lane_of((24, 128))
    out[...] = jnp.zeros_like(out)
    for t, m in enumerate((hc, ds)):
        for a in range(4):
            out[t, a, :16, :18] = m[a, :16, :]
            out[t, a, 16:, :18] = m[a, 10:18, :]
            v = out[t, a]
            out[t, a] = jnp.where(lane < 16, v, jnp.where(lane < 24, turn(v, 6), jnp.zeros_like(v)))


def coef_kernel(ids, count, wf, proj, sym, potential, last, pot, *refs):
    outs, (rows, padded, plain) = refs[:16], refs[16:]
    for x in range(4):
        v = pltpu.roll(potential[x], lax.rem(128 - 8 * ids[0], 128), 1)
        own = lane_of((16, 128)) // 8 == lax.broadcasted_iota(jnp.int32, (16, 128), 0)
        v = jnp.where(own, pltpu.roll(v, 0, 1, stride=8, stride_axis=0), jnp.zeros_like(v))
        pot[x : x + 1, :] = jnp.sum(v, axis=0, keepdims=True)

    def add(i, acc):
        p, w = [], []
        for xy in (4 * i, 4 * i + 1, 4 * i + 2, 4 * i + 3):
            p.append(jnp.concatenate([proj[pl.ds((18 * a + f) * 64 + xy, 8, stride=64), :] for a in range(4) for f in FIRST], axis=0))
            w.append(wf[pl.ds(xy, 64, stride=64), :])
        ph, plo = split(jnp.concatenate(p, axis=1))
        wh, wlo = split(jnp.concatenate(w, axis=1))
        return acc + (dot(ph, wh) + dot(ph, wlo) + dot(plo, wh))

    acc = lax.fori_loop(0, 16, add, jnp.zeros((96, 64), F32))
    row = lax.broadcasted_iota(jnp.int32, (24, 64), 0)
    slot = jnp.where(row < 16, row, row - 6)
    rows[...] = jnp.zeros_like(rows)
    plain[...] = jnp.zeros_like(plain)
    for a in range(4):
        kept = (slot < count[a]) & ((row < 16) | (slot >= 16))
        c = jnp.where(kept, acc[a * 24 : a * 24 + 24], jnp.zeros((24, 64), F32))
        padded[...] = jnp.zeros_like(padded)
        padded[:24, :] = c
        found = [c]
        for t in range(2):
            m = sym[t, a]
            right = jnp.dot(m, padded[...], precision=HI, preferred_element_type=F32)
            left = lax.dot_general(m, c, (((0,), (0,)), ((), ())), precision=HI, preferred_element_type=F32)
            found.append(0.5 * (right + left[:24]))
        for t, v in enumerate(found):
            plain[t, 18 * a : 18 * a + 16, :] = v[:16]
            plain[t, 18 * a + 16 : 18 * a + 18, :] = v[22:]
    for k in range(16):
        own = slice(5 * k, 5 * k + 5)
        rows[k, 0:5, :64] = plain[0, own, :]
        rows[k, 5:8, :64] = plain[1, 5 * k : 5 * k + 3, :]
        rows[k, 0:2, 64:] = plain[1, 5 * k + 3 : 5 * k + 5, :]
        rows[k, 2:7, 64:] = plain[2, own, :]
    lane = lane_of((8, 128))
    for m, out in zip(MOVES, outs):
        to = band_at(ids[0], m)
        out[:8, :] = rows[to]
        out[16:, :] = last[to]
        after = lax.rem(to + 1, 16)
        acc = last[after, :8, :]
        for i in range(1, 8):
            acc = jnp.where(lane % 8 == i, turn(last[after, i * 8 : i * 8 + 8, :], i), acc)
        out[8:16, :] = acc


def corr_kernel(r, pot, ah, al, part, ce, co):
    volume = 1.0 / (512 * 256)
    lane = lane_of((64, 128))
    zero = jnp.zeros((64, 128), F32)

    def prepare(g, _):
        to = pl.ds(pl.multiple_of(place(g) * 64, 64), 64)
        for x in range(3):
            cols = slice(x * 128, (x + 1) * 128)
            p = r[g, x * 64 : (x + 1) * 64, :]
            ah[to, cols], al[to, cols] = split(p)
            beside = turn(p, -8) + jnp.where(lane % 8 == 7, zero, turn(p, -1))
            if x < 2:
                beside = beside + r[g, (x + 1) * 64 : (x + 2) * 64, :]
            part[to, cols] = (1.5 + 0.5 * pot[x : x + 1, :]) * p - 0.5 * beside
        return 0

    lax.fori_loop(0, 16, prepare, 0)

    def corr(i, j):
        i, j = slice(i, i + 256), slice(j, j + 256)
        acc = dot(ah[i, :], ah[j, :]) + dot(ah[i, :], al[j, :]) + dot(al[i, :], ah[j, :])
        return acc * volume

    for q in range(2):
        for n, (i, j) in enumerate(((0, 0), (256, 0), (256, 256))):
            ce[q, n] = corr(q * 512 + i, q * 512 + j)
    for i in (0, 256):
        for j in (0, 256):
            co[i : i + 256, j : j + 256] = corr(512 + i, j)


def gram(which, ah, al, ph, lo, er, eh, es, ce, co, out, c, on):
    volume = 1.0 / (512 * 256)
    low = lane_of((64, 128)) < 64

    def ham(i, j):
        i, j = slice(i, i + 256), slice(j, j + 256)
        acc = dot(ph[i, :], ah[j, :]) + dot(ph[i, :], al[j, :]) + dot(lo[i, :], ah[j, :])
        acc += dot(ah[i, :], ph[j, :]) + dot(al[i, :], ph[j, :]) + dot(ah[i, :], lo[j, :])
        return acc + slots(eh, er, i, j)

    def corr(v, i, j):
        i, j, x = slice(i, i + 256), slice(j, j + 256), slice(384, 512)
        acc = dot(ah[i, x], ah[j, x]) + dot(ah[i, x], al[j, x]) + dot(al[i, x], ah[j, x])
        return v + acc * volume + slots(es, er, i, j)

    def tiles(e, f, t, get):
        for j in range(4):
            if f % 2:
                lower, upper = get(2 * j + 1, (f - 2 * j - 1) % 8 // 2), get(2 * j, (f - 2 * j - 1) % 8 // 2)
            else:
                lower, upper = get(2 * j, (f - 2 * j) % 8 // 2), get(2 * j + 1, (f - 2 * j - 2) % 8 // 2)
            out[e, (t + j) * 64 : (t + j) * 64 + 64, :] = jnp.where(low, lower, upper)

    @pl.when(which == 0)
    def _():
        row = lax.broadcasted_iota(jnp.int32, (256, 256), 0)
        col = lax.broadcasted_iota(jnp.int32, (256, 256), 1)
        for q in range(2):
            at = q * 512
            c[q, :256, 256:] = ham(at, at + 256)
            c[q, 256:, :256] = corr(ce[q, 1], at + 256, at)
            for n in range(2):
                here, own = slice(n * 256, n * 256 + 256), corr(ce[q, 2 * n], at + n * 256, at + n * 256)
                c[q, here, here] = jnp.where(row <= col, ham(at + n * 256, at + n * 256), own)
                diagonal = jnp.sum(jnp.where(row == col, own, jnp.zeros_like(own)), axis=0, keepdims=True)
                on[q, n] = jnp.broadcast_to(diagonal, (8, 256))
        for e in range(8):
            for q in range(2):
                tiles(e, (e - q) % 8, q * 4, lambda m, n: c[q, m * 64 : m * 64 + 64, n * 128 : n * 128 + 128])
            m = e // 2
            cols = slice(m // 2 * 128, m // 2 * 128 + 128)
            a, b = on[e % 2, 0, :, cols], on[e % 2, 1, :, cols]
            if m % 2:
                a = turn(a, 64)
            else:
                b = turn(b, 64)
            out[e, 512:, :] = jnp.where(low[:8], a, b)

    @pl.when(which == 1)
    def _():
        for i in (0, 256):
            for j in (0, 256):
                c[0, i : i + 256, j : j + 256] = ham(i, 512 + j)
                c[1, i : i + 256, j : j + 256] = corr(co[i : i + 256, j : j + 256], 512 + i, j)
        for e in range(8):
            tiles(e, e, 0, lambda m, n: c[0, m * 64 : m * 64 + 64, n * 128 : n * 128 + 128])
            tiles(e, e, 4, lambda m, n: c[1, m * 64 : m * 64 + 64, n * 128 : n * 128 + 128])
            out[e, 512:, :] = jnp.zeros((8, 128), F32)


def send_kernel(ids, part, xh, zh, pot, th, tl, ce, co, *refs):
    came, (out, ph, lo, ah, al, er, eh, es, c, on, last, cc) = refs[:16], refs[16:]
    volume = 1.0 / (512 * 256)
    lane = lane_of((64, 128))
    for m, v in zip(MOVES, came):
        g = band_at(ids[0], m, -1)
        cc[g] = v[:8, :]
        last[g] = v[8:, :]
    half = lane_of((8, 128)) < 64
    none = jnp.zeros((3, 128), F32)
    for n in range(8):
        a, b = cc[4 * n % 16 + n // 4], cc[(4 * n + 2) % 16 + n // 4]
        x, y = jnp.where(half, a, turn(b, 64)), jnp.where(half, turn(a, 64), b)
        for t, (e, v) in enumerate(((er, x[:5]), (eh, jnp.concatenate([x[5:], y[:2]], axis=0)), (es, y[2:7]))):
            hi, mid = [w.astype(F32) for w in split(jnp.concatenate([v, none], axis=0))]
            zero = jnp.zeros_like(hi)
            terms = [hi, hi, mid, zero] if t else [hi, mid, hi, zero]
            e[:, n * 128 : n * 128 + 128] = jnp.concatenate(terms, axis=0).astype(BF16)

    def prepare(g, _):
        to = pl.ds(pl.multiple_of(place(g) * 64, 64), 64)
        two = zh[g]
        ext = jnp.concatenate([two, turn(two, -4)], axis=0)
        end = lane % 8 == 7
        p = last[g, 8:, :]
        ah[to, :384], al[to, :384] = th[to, :], tl[to, :]
        ah[to, 384:], al[to, 384:] = split(p)
        for x in range(3):
            cols = slice(x * 128, (x + 1) * 128)
            beside = jnp.where(end, turn(ext, 7 - x), jnp.zeros((64, 128), F32))
            if x == 2:
                beside = beside + p
            ph[to, cols], lo[to, cols] = split((part[to, cols] - 0.5 * beside) * volume)
        after = last[g, :8, :]
        after = jnp.concatenate([turn(after, 7 - i) for i in range(8)], axis=0)
        beside = xh[g] + turn(p, -8) + jnp.where(end, after, turn(p, -1))
        phi = (1.5 + 0.5 * pot[3:4, :]) * p - 0.5 * beside
        ph[to, 384:], lo[to, 384:] = split(phi * volume)
        return 0

    lax.fori_loop(0, 16, prepare, 0)
    gram(1 - lax.rem(ids[1], 2), ah, al, ph, lo, er, eh, es, ce, co, out, c, on)


def keep_kernel(ids, ph, lo, ah, al, er, eh, es, ce, co, out, c, on):
    gram(lax.rem(ids[1], 2), ah, al, ph, lo, er, eh, es, ce, co, out, c, on)


def first_kernel(ids, keep, mate, s1, s2, s3, own):
    d = ids[1]
    north, x, h = lax.rem(d, 2) == 1, d // 4, lax.rem(d // 2, 2)

    def total(ref, i, across, along):
        e = jnp.where(north, along, across)
        ref[i] = keep[e] + mate[e]

    def part(dx, y):
        return lax.rem(x + dx, 4) * 2 + y

    for i in range(2):
        total(s1, i, part(1, i), part(i, 1 - h))
        total(s2, i, part(3, i), part(2 + i, 1 - h))
        total(own, i, part(0, i), part(i, h))
        total(own, 2 + i, part(0, i), part(2 + i, h))
        total(s3, i, part(2, i), part(2, i))


def second_kernel(ids, own, r1, r2, r3, keep, s1, s2, s3):
    d = ids[1]
    north, h = lax.rem(d, 2) == 1, lax.rem(d // 2, 2)

    @pl.when(jnp.logical_not(north))
    def _():
        def total(i):
            return own[i] + r1[i] + r2[i] + r3[i]

        keep[...] = total(h)
        s1[...] = total(1 - h)

    @pl.when(north)
    def _():
        keep[...] = own[0] + r1[0]
        s1[...] = own[1] + r1[1]
        s3[...] = own[2] + r2[0]
        s2[...] = own[3] + r2[1]


def rows_kernel(ids, keep, r1, r2, r3, out, total):
    d = ids[1]
    low = lane_of((64, 128)) < 64
    total[...] = keep[...] + r1[...]

    @pl.when(lax.rem(d, 2) == 1)
    def _():
        total[...] = total[...] + (r2[...] + r3[...])

    e = d // 2
    even = 1 - lax.rem(d, 2)

    def block(g, upper):
        m, p = g // 2, lax.rem(g, 2)
        t = total[pl.ds(pl.multiple_of((p * 4 + m // 2) * 64, 64), 64), :]
        half = lax.rem(m + e + even * p, 2)
        return jnp.where(half == upper, t, pltpu.roll(t, 64, 1))

    for g in range(16):
        h = lax.rem(d - g + 16, 16)
        own = jnp.broadcast_to(total[512:513, :], (64, 128))
        own = own if g >= 8 else turn(own, 64)
        out[g] = jnp.where(low, block(jnp.int32(g), 0), jnp.where(h == g, own, block(h, 1)))


def finish_kernel(ids, parts, out):
    b, d = ids[0], ids[1]
    h = lax.rem(d - b + 16, 16)
    t = parts[0]
    for s in range(1, 16):
        t = t + parts[s]
    low = lane_of((64, 128)) < 64
    both = jnp.concatenate([t, t], axis=0).T
    left, right, other = both[:64], both[64:], turn(t, 64)
    upper = jnp.where(low, t, right)
    lower = jnp.where(low, right, other)
    row, col = lax.broadcasted_iota(jnp.int32, (64, 128), 0), lane_of((64, 128)) % 64
    own = jnp.where(low, jnp.where(row <= col, t, left), jnp.where(row > col, other, jnp.where(row < col, left, t)))
    first = jnp.where(lax.rem(d, 2) == 1, lax.rem(b, 2), (b > h).astype(jnp.int32)) == 0
    out[...] = jnp.where(b == h, own, jnp.where(first, upper, lower))


def join_kernel(a, b, c, d, out):
    for i, v in enumerate((a, b, c, d)):
        out[i] = v[...]


def assemble_kernel(ids, own, r1, r2, r3, ham, corr, parts):
    b, d = ids[0], ids[1]
    low = lane_of((64, 128)) < 64
    for i, v in enumerate((own, r1, r2, r3)):
        parts[4 * i : 4 * i + 4] = v[...]

    def piece(h):
        at = lax.rem(h + b, 16)
        ahead = lax.rem(at // 4 - d // 4 + 4, 4)
        return parts[ahead * 4 + (lax.rem(at, 4) ^ lax.rem(d, 4))]

    for j in range(8):
        t0, t1 = piece(2 * j), piece(2 * j + 1)
        cols = slice(j * 128, (j + 1) * 128)
        ham[:, cols] = jnp.where(low, t0, turn(t1, 64))
        corr[:, cols] = jnp.where(low, turn(t0, 64), t1)


def call(kernel, args, outs, scratch=(), flops=0, mib=8):
    specs = [SMEM if a.dtype == jnp.int32 else VMEM for a in args]
    size = sum(a.size * a.dtype.itemsize for a in (*args, *outs))
    single = len(outs) == 1
    return pl.pallas_call(
        kernel,
        out_shape=outs[0] if single else outs,
        in_specs=specs,
        out_specs=VMEM if single else [VMEM] * len(outs),
        scratch_shapes=scratch,
        compiler_params=pltpu.CompilerParams(vmem_limit_bytes=mib * 1024 * 1024),
        cost_estimate=pl.CostEstimate(flops=flops or 8 * size, bytes_accessed=size, transcendentals=0),
    )(*args)


def shape(*dims, dtype=F32):
    return jax.ShapeDtypeStruct(dims, dtype)


def moves(south, north):
    pairs = []
    for d in range(16):
        x, h, c = d // 4, d // 2 % 2, d % 2
        step = north if c else south
        if step:
            pairs.append((d, (x + step[0]) % 4 * 4 + (h + step[1]) % 2 * 2 + c))
    return pairs


def reduced_over_dom(ids, keep, mate):
    piece = (520, 128)
    sends = call(first_kernel, (ids, keep, mate), [shape(n, *piece) for n in (2, 2, 2, 4)], mib=16)
    steps = (((1, 0), (0, 1)), ((3, 0), (0, 1)), ((2, 0), None))
    got = [lax.ppermute(v, "dom", moves(*s)) for v, s in zip(sends, steps)]
    keep, *sends = call(second_kernel, (ids, sends[3], *got), [shape(*piece)] * 4, mib=12)
    steps = (((0, 1), (1, 0)), (None, (3, 0)), (None, (2, 0)))
    got = [lax.ppermute(v, "dom", moves(*s)) for v, s in zip(sends, steps)]
    return call(rows_kernel, (ids, keep, *got), (shape(16, 64, 128),), [pltpu.VMEM(piece, F32)], mib=8)


def on_device(wavefunctions, potential, projectors, hamiltonian_correction, delta_s, projector_count):
    bands, cx, ny, nz = wavefunctions.shape
    atoms, slots = hamiltonian_correction.shape[:2]
    b, d = lax.axis_index("band"), lax.axis_index("dom")
    ids = jnp.stack([b, d]).astype(jnp.int32)

    flat = cx * ny
    wf = wavefunctions.reshape(bands * flat, nz)
    parts, last = pl.pallas_call(
        spread_kernel,
        out_shape=[shape(16, 3 * bands, 128), shape(16, bands, 128)],
        in_specs=[pl.BlockSpec(memory_space=pltpu.HBM)],
        out_specs=[pl.BlockSpec(memory_space=pltpu.HBM)] * 2,
        scratch_shapes=[
            pltpu.VMEM((bands * flat, nz), F32),
            pltpu.VMEM((16, cx * bands, 128), F32),
            pltpu.SemaphoreType.DMA((10,)),
        ],
        compiler_params=pltpu.CompilerParams(vmem_limit_bytes=61 * 1024 * 1024),
    )(wf)
    slab = lax.all_to_all(parts, "band", 0, 0, tiled=True)

    proj = projectors.reshape(atoms * slots * flat, nz)
    wf, proj, potential, hamiltonian_correction, delta_s, parts = lax.optimization_barrier(
        (wf, proj, potential, hamiltonian_correction, delta_s, parts)
    )
    sym = call(couple_kernel, (hamiltonian_correction, delta_s), (shape(2, atoms, 24, 128),), mib=2)
    pot, *came = call(
        coef_kernel,
        (ids, projector_count, wf, proj, sym, potential, last),
        [shape(cx, nz)] + [shape(16 + bands, 128)] * 16,
        [pltpu.VMEM((16, 8, 128), F32), pltpu.VMEM((128, bands), F32), pltpu.VMEM((3, 80, bands), F32)],
    )
    for i, move in enumerate(MOVES):
        if i:
            came[i] = lax.ppermute(came[i], "band", [(j, band_at(j, move)) for j in range(16)])
    back = [((i + 1) % 16, i) for i in range(16)]
    first, below = call(edge_kernel, (slab,), [shape(16, bands, 128), shape(16, bands // 2, 128)], mib=4)
    ahead, above = lax.ppermute(first, "dom", back), lax.ppermute(below, "band", back)
    m = 16 * bands
    three, wide = shape(m, 384, dtype=BF16), shape(m, 512, dtype=BF16)
    ext = [shape(32, m, dtype=BF16)] * 3
    work = 2 * m * m * 512
    quads = [pltpu.VMEM((2, 512, 512), F32), pltpu.VMEM((2, 2, 8, 256), F32)]
    ah, al, part, ce, co = call(
        corr_kernel,
        (slab, pot),
        [three, three, shape(m, 384), shape(2, 3, 256, 256), shape(512, 512)],
        flops=3 * work,
        mib=16,
    )
    ahead, above, ah, *came = lax.optimization_barrier((ahead, above, ah, *came))
    parts = shape(8, 520, 128)
    send, *rest = call(
        send_kernel,
        (ids, part, ahead, above, pot, ah, al, ce, co, *came),
        [parts, wide, wide, wide, wide, *ext],
        quads + [pltpu.VMEM((16, 72, 128), F32), pltpu.VMEM((16, 8, 128), F32)],
        3 * work,
        22,
    )
    mate = lax.ppermute(send, "dom", [(i, i ^ 1) for i in range(16)])
    keep = call(keep_kernel, (ids, *rest, ce, co), [parts], quads, 3 * work, 18)
    parts = reduced_over_dom(ids, keep, mate)
    parts = lax.all_to_all(parts, "band", 0, 0, tiled=True)
    own = call(finish_kernel, (ids, parts), (shape(64, 128),))
    near = [lax.ppermute(own, "dom", [(i, i ^ j) for i in range(16)]) for j in (1, 2, 3)]
    own = call(join_kernel, (own, *near), (shape(4, 64, 128),))
    far = [lax.ppermute(own, "dom", [((i + 4 * j) % 16, i) for i in range(16)]) for j in (1, 2, 3)]
    return call(
        assemble_kernel,
        (ids, own, *far),
        (shape(64, 1024), shape(64, 1024)),
        [pltpu.VMEM((16, 64, 128), F32)],
    )


def solution(mesh):
    placed = (
        P("band", "dom", None, None),
        P("dom", None, None),
        P("dom", None, None, None, None),
        P("dom", None, None),
        P("dom", None, None),
        P("dom"),
    )
    return jax.shard_map(
        on_device,
        mesh=mesh,
        in_specs=placed,
        out_specs=(P("band", None), P("band", None)),
        check_vma=False,
    )
```

```python
import jax
import jax.numpy as jnp
from jax import lax
from jax.experimental import pallas as pl
from jax.experimental.pallas import tpu as pltpu
from jax.sharding import PartitionSpec as P


F32 = jnp.float32
BF16 = jnp.bfloat16
HI = lax.Precision.HIGHEST
VMEM = pl.BlockSpec(memory_space=pltpu.VMEM)
SMEM = pl.BlockSpec(memory_space=pltpu.SMEM)


def lane_of(shape):
    return lax.broadcasted_iota(jnp.int32, shape, len(shape) - 1)


def turn(x, n):
    n = n % 128
    return pltpu.roll(x, n, 1) if n else x


MOVES = [(0, 0)] + [(y, z) for z in (4, 3, -3, 2, -2, 1, -1) for y in (0, 1)] + [(1, 0)]


def band_at(b, move, sign=1):
    return (b // 8 + move[0]) % 2 * 8 + (b + sign * move[1] + 8) % 8


def spread_kernel(wf, out, last, held, ready, sems):
    lane = lane_of((8, 128))
    block = lane // 8

    def fetch(i):
        rows = pl.ds(pl.multiple_of(i * 512, 512), 512)
        return pltpu.make_async_copy(wf.at[rows], held.at[rows], sems.at[i])

    for i in range(8):
        fetch(i).start()

    def body(bg, _):
        fetch(bg).wait()
        for x in range(4):
            v = [held[pl.ds(bg * 512 + x * 16 + y, 8, stride=64), :] for y in range(16)]
            for s in (1, 2, 4, 8):
                low = (block & s) == 0
                nxt = list(v)
                for y in range(16):
                    if not y & s:
                        a, b = v[y], v[y + s]
                        if s == 8:
                            a_high = b_low = turn(jnp.where(low, b, a), 64)
                        else:
                            b_low, a_high = turn(b, s * 8), turn(a, -s * 8)
                        nxt[y] = jnp.where(low, a, b_low)
                        nxt[y + s] = jnp.where(low, a_high, b)
                v = nxt
            rows = pl.ds(pl.multiple_of(x * 64 + bg * 8, 8), 8)
            for k in range(16):
                ready[k, rows, :] = v[k]
        return 0

    lax.fori_loop(0, 8, body, 0)
    one = pltpu.make_async_copy(ready.at[:, :192], out, sems.at[8])
    two = pltpu.make_async_copy(ready.at[:, 192:], last, sems.at[9])
    one.start()
    two.start()
    one.wait()
    two.wait()


def plane_kernel(r, out):
    out[...] = r[...]


def edge_kernel(r, below):
    lane = lane_of((32, 128))

    def body(g, _):
        acc = r[g, :32, :]
        for i in (1, 2, 4, 5, 6):
            at = i % 4 * 64 + i // 4 * 32
            acc = jnp.where(lane % 8 == i, turn(r[g, at : at + 32, :], i), acc)
        below[g] = acc
        return 0

    lax.fori_loop(0, 16, body, 0)


def split(x):
    hi = x.astype(BF16)
    return hi, (x - hi.astype(F32)).astype(BF16)


def dot(a, b):
    return lax.dot_general(a, b, (((1,), (1,)), ((), ())), preferred_element_type=F32)


def slots(e, er, i, j):
    return lax.dot_general(e[:, i], er[:, j], (((0,), (0,)), ((), ())), preferred_element_type=F32)


def place(g):
    return (g % 2) * 8 + g // 2


FIRST = (0, 8, 10)


def couple_kernel(hc, ds, out):
    lane = lane_of((24, 128))
    out[...] = jnp.zeros_like(out)
    for t, m in enumerate((hc, ds)):
        for a in range(4):
            out[t, a, :16, :18] = m[a, :16, :]
            out[t, a, 16:, :18] = m[a, 10:18, :]
            v = out[t, a]
            out[t, a] = jnp.where(lane < 16, v, jnp.where(lane < 24, turn(v, 6), jnp.zeros_like(v)))


def coef_kernel(ids, count, wf, proj, sym, potential, last, pot, *refs):
    outs, (rows, padded, plain) = refs[:16], refs[16:]
    for x in range(4):
        v = pltpu.roll(potential[x], lax.rem(128 - 8 * ids[0], 128), 1)
        own = lane_of((16, 128)) // 8 == lax.broadcasted_iota(jnp.int32, (16, 128), 0)
        v = jnp.where(own, pltpu.roll(v, 0, 1, stride=8, stride_axis=0), jnp.zeros_like(v))
        pot[x : x + 1, :] = jnp.sum(v, axis=0, keepdims=True)

    def add(i, acc):
        p, w = [], []
        for xy in (4 * i, 4 * i + 1, 4 * i + 2, 4 * i + 3):
            p.append(jnp.concatenate([proj[pl.ds((18 * a + f) * 64 + xy, 8, stride=64), :] for a in range(4) for f in FIRST], axis=0))
            w.append(wf[pl.ds(xy, 64, stride=64), :])
        ph, plo = split(jnp.concatenate(p, axis=1))
        wh, wlo = split(jnp.concatenate(w, axis=1))
        return acc + (dot(ph, wh) + dot(ph, wlo) + dot(plo, wh))

    acc = lax.fori_loop(0, 16, add, jnp.zeros((96, 64), F32))
    row = lax.broadcasted_iota(jnp.int32, (24, 64), 0)
    slot = jnp.where(row < 16, row, row - 6)
    rows[...] = jnp.zeros_like(rows)
    plain[...] = jnp.zeros_like(plain)
    for a in range(4):
        kept = (slot < count[a]) & ((row < 16) | (slot >= 16))
        c = jnp.where(kept, acc[a * 24 : a * 24 + 24], jnp.zeros((24, 64), F32))
        padded[...] = jnp.zeros_like(padded)
        padded[:24, :] = c
        found = [c]
        for t in range(2):
            m = sym[t, a]
            right = jnp.dot(m, padded[...], precision=HI, preferred_element_type=F32)
            left = lax.dot_general(m, c, (((0,), (0,)), ((), ())), precision=HI, preferred_element_type=F32)
            found.append(0.5 * (right + left[:24]))
        for t, v in enumerate(found):
            plain[t, 18 * a : 18 * a + 16, :] = v[:16]
            plain[t, 18 * a + 16 : 18 * a + 18, :] = v[22:]
    for k in range(16):
        own = slice(5 * k, 5 * k + 5)
        rows[k, 0:5, :64] = plain[0, own, :]
        rows[k, 5:8, :64] = plain[1, 5 * k : 5 * k + 3, :]
        rows[k, 0:2, 64:] = plain[1, 5 * k + 3 : 5 * k + 5, :]
        rows[k, 2:7, 64:] = plain[2, own, :]
    lane = lane_of((8, 128))
    for m, out in zip(MOVES, outs):
        to = band_at(ids[0], m)
        out[:8, :] = rows[to]
        out[16:, :] = last[to]
        after = lax.rem(to + 1, 16)
        acc = last[after, :8, :]
        for i in range(1, 8):
            acc = jnp.where(lane % 8 == i, turn(last[after, i * 8 : i * 8 + 8, :], i), acc)
        out[8:16, :] = acc


def corr_kernel(r, pot, ah, al, part, ce, co):
    volume = 1.0 / (512 * 256)
    lane = lane_of((64, 128))
    zero = jnp.zeros((64, 128), F32)

    def prepare(g, _):
        to = pl.ds(pl.multiple_of(place(g) * 64, 64), 64)
        for x in range(3):
            cols = slice(x * 128, (x + 1) * 128)
            p = r[g, x * 64 : (x + 1) * 64, :]
            ah[to, cols], al[to, cols] = split(p)
            beside = turn(p, -8) + jnp.where(lane % 8 == 7, zero, turn(p, -1))
            if x < 2:
                beside = beside + r[g, (x + 1) * 64 : (x + 2) * 64, :]
            part[to, cols] = (1.5 + 0.5 * pot[x : x + 1, :]) * p - 0.5 * beside
        return 0

    lax.fori_loop(0, 16, prepare, 0)

    def corr(i, j):
        i, j = slice(i, i + 256), slice(j, j + 256)
        acc = dot(ah[i, :], ah[j, :]) + dot(ah[i, :], al[j, :]) + dot(al[i, :], ah[j, :])
        return acc * volume

    for q in range(2):
        for n, (i, j) in enumerate(((0, 0), (256, 0), (256, 256))):
            ce[q, n] = corr(q * 512 + i, q * 512 + j)
    for i in (0, 256):
        for j in (0, 256):
            co[i : i + 256, j : j + 256] = corr(512 + i, j)


def gram(which, ah, al, ph, lo, er, eh, es, ce, co, out, c, on):
    volume = 1.0 / (512 * 256)
    low = lane_of((64, 128)) < 64

    def ham(i, j):
        i, j = slice(i, i + 256), slice(j, j + 256)
        acc = dot(ph[i, :], ah[j, :]) + dot(ph[i, :], al[j, :]) + dot(lo[i, :], ah[j, :])
        acc += dot(ah[i, :], ph[j, :]) + dot(al[i, :], ph[j, :]) + dot(ah[i, :], lo[j, :])
        return acc + slots(eh, er, i, j)

    def corr(v, i, j):
        i, j, x = slice(i, i + 256), slice(j, j + 256), slice(384, 512)
        acc = dot(ah[i, x], ah[j, x]) + dot(ah[i, x], al[j, x]) + dot(al[i, x], ah[j, x])
        return v + acc * volume + slots(es, er, i, j)

    def tiles(e, f, t, get):
        for j in range(4):
            if f % 2:
                lower, upper = get(2 * j + 1, (f - 2 * j - 1) % 8 // 2), get(2 * j, (f - 2 * j - 1) % 8 // 2)
            else:
                lower, upper = get(2 * j, (f - 2 * j) % 8 // 2), get(2 * j + 1, (f - 2 * j - 2) % 8 // 2)
            out[e, (t + j) * 64 : (t + j) * 64 + 64, :] = jnp.where(low, lower, upper)

    @pl.when(which == 0)
    def _():
        row = lax.broadcasted_iota(jnp.int32, (256, 256), 0)
        col = lax.broadcasted_iota(jnp.int32, (256, 256), 1)
        for q in range(2):
            at = q * 512
            c[q, :256, 256:] = ham(at, at + 256)
            c[q, 256:, :256] = corr(ce[q, 1], at + 256, at)
            for n in range(2):
                here, own = slice(n * 256, n * 256 + 256), corr(ce[q, 2 * n], at + n * 256, at + n * 256)
                c[q, here, here] = jnp.where(row <= col, ham(at + n * 256, at + n * 256), own)
                diagonal = jnp.sum(jnp.where(row == col, own, jnp.zeros_like(own)), axis=0, keepdims=True)
                on[q, n] = jnp.broadcast_to(diagonal, (8, 256))
        for e in range(8):
            for q in range(2):
                tiles(e, (e - q) % 8, q * 4, lambda m, n: c[q, m * 64 : m * 64 + 64, n * 128 : n * 128 + 128])
            m = e // 2
            cols = slice(m // 2 * 128, m // 2 * 128 + 128)
            a, b = on[e % 2, 0, :, cols], on[e % 2, 1, :, cols]
            if m % 2:
                a = turn(a, 64)
            else:
                b = turn(b, 64)
            out[e, 512:, :] = jnp.where(low[:8], a, b)

    @pl.when(which == 1)
    def _():
        for i in (0, 256):
            for j in (0, 256):
                c[0, i : i + 256, j : j + 256] = ham(i, 512 + j)
                c[1, i : i + 256, j : j + 256] = corr(co[i : i + 256, j : j + 256], 512 + i, j)
        for e in range(8):
            tiles(e, e, 0, lambda m, n: c[0, m * 64 : m * 64 + 64, n * 128 : n * 128 + 128])
            tiles(e, e, 4, lambda m, n: c[1, m * 64 : m * 64 + 64, n * 128 : n * 128 + 128])
            out[e, 512:, :] = jnp.zeros((8, 128), F32)


def send_kernel(ids, part, xh, zh, pot, th, tl, ce, co, *refs):
    came, (out, ph, lo, ah, al, er, eh, es, c, on, last, cc) = refs[:16], refs[16:]
    volume = 1.0 / (512 * 256)
    lane = lane_of((64, 128))
    for m, v in zip(MOVES, came):
        g = band_at(ids[0], m, -1)
        cc[g] = v[:8, :]
        last[g] = v[8:, :]
    half = lane_of((8, 128)) < 64
    none = jnp.zeros((3, 128), F32)
    for n in range(8):
        a, b = cc[4 * n % 16 + n // 4], cc[(4 * n + 2) % 16 + n // 4]
        x, y = jnp.where(half, a, turn(b, 64)), jnp.where(half, turn(a, 64), b)
        for t, (e, v) in enumerate(((er, x[:5]), (eh, jnp.concatenate([x[5:], y[:2]], axis=0)), (es, y[2:7]))):
            hi, mid = [w.astype(F32) for w in split(jnp.concatenate([v, none], axis=0))]
            zero = jnp.zeros_like(hi)
            terms = [hi, hi, mid, zero] if t else [hi, mid, hi, zero]
            e[:, n * 128 : n * 128 + 128] = jnp.concatenate(terms, axis=0).astype(BF16)

    def prepare(g, _):
        to = pl.ds(pl.multiple_of(place(g) * 64, 64), 64)
        two = zh[g]
        ext = jnp.concatenate([two, turn(two, -4)], axis=0)
        end = lane % 8 == 7
        p = last[g, 8:, :]
        ah[to, :384], al[to, :384] = th[to, :], tl[to, :]
        ah[to, 384:], al[to, 384:] = split(p)
        for x in range(3):
            cols = slice(x * 128, (x + 1) * 128)
            beside = jnp.where(end, turn(ext, 7 - x), jnp.zeros((64, 128), F32))
            if x == 2:
                beside = beside + p
            ph[to, cols], lo[to, cols] = split((part[to, cols] - 0.5 * beside) * volume)
        after = last[g, :8, :]
        after = jnp.concatenate([turn(after, 7 - i) for i in range(8)], axis=0)
        beside = xh[g] + turn(p, -8) + jnp.where(end, after, turn(p, -1))
        phi = (1.5 + 0.5 * pot[3:4, :]) * p - 0.5 * beside
        ph[to, 384:], lo[to, 384:] = split(phi * volume)
        return 0

    lax.fori_loop(0, 16, prepare, 0)
    gram(1 - lax.rem(ids[1], 2), ah, al, ph, lo, er, eh, es, ce, co, out, c, on)


def keep_kernel(ids, ph, lo, ah, al, er, eh, es, ce, co, out, c, on):
    gram(lax.rem(ids[1], 2), ah, al, ph, lo, er, eh, es, ce, co, out, c, on)


def first_kernel(ids, keep, mate, s1, s2, s3, own):
    d = ids[1]
    north, x, h = lax.rem(d, 2) == 1, d // 4, lax.rem(d // 2, 2)

    def total(ref, i, across, along):
        e = jnp.where(north, along, across)
        ref[i] = keep[e] + mate[e]

    def part(dx, y):
        return lax.rem(x + dx, 4) * 2 + y

    for i in range(2):
        total(s1, i, part(1, i), part(i, 1 - h))
        total(s2, i, part(3, i), part(2 + i, 1 - h))
        total(own, i, part(0, i), part(i, h))
        total(own, 2 + i, part(0, i), part(2 + i, h))
        total(s3, i, part(2, i), part(2, i))


def second_kernel(ids, own, r1, r2, r3, keep, s1, s2, s3):
    d = ids[1]
    north, h = lax.rem(d, 2) == 1, lax.rem(d // 2, 2)

    @pl.when(jnp.logical_not(north))
    def _():
        def total(i):
            return own[i] + r1[i] + r2[i] + r3[i]

        keep[...] = total(h)
        s1[...] = total(1 - h)

    @pl.when(north)
    def _():
        keep[...] = own[0] + r1[0]
        s1[...] = own[1] + r1[1]
        s3[...] = own[2] + r2[0]
        s2[...] = own[3] + r2[1]


def rows_kernel(ids, keep, r1, r2, r3, out, total):
    d = ids[1]
    low = lane_of((64, 128)) < 64
    total[...] = keep[...] + r1[...]

    @pl.when(lax.rem(d, 2) == 1)
    def _():
        total[...] = total[...] + (r2[...] + r3[...])

    e = d // 2
    even = 1 - lax.rem(d, 2)

    def block(g, upper):
        m, p = g // 2, lax.rem(g, 2)
        t = total[pl.ds(pl.multiple_of((p * 4 + m // 2) * 64, 64), 64), :]
        half = lax.rem(m + e + even * p, 2)
        return jnp.where(half == upper, t, pltpu.roll(t, 64, 1))

    for g in range(16):
        h = lax.rem(d - g + 16, 16)
        own = jnp.broadcast_to(total[512:513, :], (64, 128))
        own = own if g >= 8 else turn(own, 64)
        out[g] = jnp.where(low, block(jnp.int32(g), 0), jnp.where(h == g, own, block(h, 1)))


def finish_kernel(ids, parts, out):
    b, d = ids[0], ids[1]
    h = lax.rem(d - b + 16, 16)
    t = parts[0]
    for s in range(1, 16):
        t = t + parts[s]
    low = lane_of((64, 128)) < 64
    both = jnp.concatenate([t, t], axis=0).T
    left, right, other = both[:64], both[64:], turn(t, 64)
    upper = jnp.where(low, t, right)
    lower = jnp.where(low, right, other)
    row, col = lax.broadcasted_iota(jnp.int32, (64, 128), 0), lane_of((64, 128)) % 64
    own = jnp.where(low, jnp.where(row <= col, t, left), jnp.where(row > col, other, jnp.where(row < col, left, t)))
    first = jnp.where(lax.rem(d, 2) == 1, lax.rem(b, 2), (b > h).astype(jnp.int32)) == 0
    out[...] = jnp.where(b == h, own, jnp.where(first, upper, lower))


def join_kernel(a, b, c, d, out):
    for i, v in enumerate((a, b, c, d)):
        out[i] = v[...]


def assemble_kernel(ids, own, r1, r2, r3, ham, corr, parts):
    b, d = ids[0], ids[1]
    low = lane_of((64, 128)) < 64
    for i, v in enumerate((own, r1, r2, r3)):
        parts[4 * i : 4 * i + 4] = v[...]

    def piece(h):
        at = lax.rem(h + b, 16)
        ahead = lax.rem(at // 4 - d // 4 + 4, 4)
        return parts[ahead * 4 + (lax.rem(at, 4) ^ lax.rem(d, 4))]

    for j in range(8):
        t0, t1 = piece(2 * j), piece(2 * j + 1)
        cols = slice(j * 128, (j + 1) * 128)
        ham[:, cols] = jnp.where(low, t0, turn(t1, 64))
        corr[:, cols] = jnp.where(low, turn(t0, 64), t1)


def call(kernel, args, outs, scratch=(), flops=0, mib=8):
    specs = [SMEM if a.dtype == jnp.int32 else VMEM for a in args]
    size = sum(a.size * a.dtype.itemsize for a in (*args, *outs))
    single = len(outs) == 1
    return pl.pallas_call(
        kernel,
        out_shape=outs[0] if single else outs,
        in_specs=specs,
        out_specs=VMEM if single else [VMEM] * len(outs),
        scratch_shapes=scratch,
        compiler_params=pltpu.CompilerParams(vmem_limit_bytes=mib * 1024 * 1024),
        cost_estimate=pl.CostEstimate(flops=flops or 8 * size, bytes_accessed=size, transcendentals=0),
    )(*args)


def shape(*dims, dtype=F32):
    return jax.ShapeDtypeStruct(dims, dtype)


def moves(south, north):
    pairs = []
    for d in range(16):
        x, h, c = d // 4, d // 2 % 2, d % 2
        step = north if c else south
        if step:
            pairs.append((d, (x + step[0]) % 4 * 4 + (h + step[1]) % 2 * 2 + c))
    return pairs


def reduced_over_dom(ids, keep, mate):
    piece = (520, 128)
    sends = call(first_kernel, (ids, keep, mate), [shape(n, *piece) for n in (2, 2, 2, 4)], mib=16)
    steps = (((1, 0), (0, 1)), ((3, 0), (0, 1)), ((2, 0), None))
    got = [lax.ppermute(v, "dom", moves(*s)) for v, s in zip(sends, steps)]
    keep, *sends = call(second_kernel, (ids, sends[3], *got), [shape(*piece)] * 4, mib=12)
    steps = (((0, 1), (1, 0)), (None, (3, 0)), (None, (2, 0)))
    got = [lax.ppermute(v, "dom", moves(*s)) for v, s in zip(sends, steps)]
    return call(rows_kernel, (ids, keep, *got), (shape(16, 64, 128),), [pltpu.VMEM(piece, F32)], mib=8)


def on_device(wavefunctions, potential, projectors, hamiltonian_correction, delta_s, projector_count):
    bands, cx, ny, nz = wavefunctions.shape
    atoms, slots = hamiltonian_correction.shape[:2]
    b, d = lax.axis_index("band"), lax.axis_index("dom")
    ids = jnp.stack([b, d]).astype(jnp.int32)

    flat = cx * ny
    wf = wavefunctions.reshape(bands * flat, nz)
    parts, last = pl.pallas_call(
        spread_kernel,
        out_shape=[shape(16, 3 * bands, 128), shape(16, bands, 128)],
        in_specs=[pl.BlockSpec(memory_space=pltpu.HBM)],
        out_specs=[pl.BlockSpec(memory_space=pltpu.HBM)] * 2,
        scratch_shapes=[
            pltpu.VMEM((bands * flat, nz), F32),
            pltpu.VMEM((16, cx * bands, 128), F32),
            pltpu.SemaphoreType.DMA((10,)),
        ],
        compiler_params=pltpu.CompilerParams(vmem_limit_bytes=61 * 1024 * 1024),
    )(wf)
    slab = lax.all_to_all(parts, "band", 0, 0, tiled=True)

    proj = projectors.reshape(atoms * slots * flat, nz)
    wf, proj, potential, hamiltonian_correction, delta_s, parts = lax.optimization_barrier(
        (wf, proj, potential, hamiltonian_correction, delta_s, parts)
    )
    sym = call(couple_kernel, (hamiltonian_correction, delta_s), (shape(2, atoms, 24, 128),), mib=2)
    pot, *came = call(
        coef_kernel,
        (ids, projector_count, wf, proj, sym, potential, last),
        [shape(cx, nz)] + [shape(16 + bands, 128)] * 16,
        [pltpu.VMEM((16, 8, 128), F32), pltpu.VMEM((128, bands), F32), pltpu.VMEM((3, 80, bands), F32)],
    )
    for i, move in enumerate(MOVES):
        if i:
            came[i] = lax.ppermute(came[i], "band", [(j, band_at(j, move)) for j in range(16)])
    back = [((i + 1) % 16, i) for i in range(16)]
    first = pl.pallas_call(
        plane_kernel,
        grid=(1,),
        out_shape=shape(16, bands, 128),
        in_specs=[pl.BlockSpec((16, bands, 128), lambda i: (0, 0, 0))],
        out_specs=pl.BlockSpec((16, bands, 128), lambda i: (0, 0, 0)),
        compiler_params=pltpu.CompilerParams(vmem_limit_bytes=4 * 1024 * 1024),
        cost_estimate=pl.CostEstimate(flops=1000, bytes_accessed=2**20, transcendentals=0),
    )(slab)
    below = call(edge_kernel, (slab,), [shape(16, bands // 2, 128)], mib=4)
    ahead, above = lax.ppermute(first, "dom", back), lax.ppermute(below, "band", back)
    m = 16 * bands
    three, wide = shape(m, 384, dtype=BF16), shape(m, 512, dtype=BF16)
    ext = [shape(32, m, dtype=BF16)] * 3
    work = 2 * m * m * 512
    quads = [pltpu.VMEM((2, 512, 512), F32), pltpu.VMEM((2, 2, 8, 256), F32)]
    ah, al, part, ce, co = call(
        corr_kernel,
        (slab, pot),
        [three, three, shape(m, 384), shape(2, 3, 256, 256), shape(512, 512)],
        flops=3 * work,
        mib=16,
    )
    ahead, above, ah, *came = lax.optimization_barrier((ahead, above, ah, *came))
    parts = shape(8, 520, 128)
    send, *rest = call(
        send_kernel,
        (ids, part, ahead, above, pot, ah, al, ce, co, *came),
        [parts, wide, wide, wide, wide, *ext],
        quads + [pltpu.VMEM((16, 72, 128), F32), pltpu.VMEM((16, 8, 128), F32)],
        3 * work,
        22,
    )
    mate = lax.ppermute(send, "dom", [(i, i ^ 1) for i in range(16)])
    keep = call(keep_kernel, (ids, *rest, ce, co), [parts], quads, 3 * work, 18)
    parts = reduced_over_dom(ids, keep, mate)
    parts = lax.all_to_all(parts, "band", 0, 0, tiled=True)
    own = call(finish_kernel, (ids, parts), (shape(64, 128),))
    near = [lax.ppermute(own, "dom", [(i, i ^ j) for i in range(16)]) for j in (1, 2, 3)]
    own = call(join_kernel, (own, *near), (shape(4, 64, 128),))
    far = [lax.ppermute(own, "dom", [((i + 4 * j) % 16, i) for i in range(16)]) for j in (1, 2, 3)]
    return call(
        assemble_kernel,
        (ids, own, *far),
        (shape(64, 1024), shape(64, 1024)),
        [pltpu.VMEM((16, 64, 128), F32)],
    )


def solution(mesh):
    placed = (
        P("band", "dom", None, None),
        P("dom", None, None),
        P("dom", None, None, None, None),
        P("dom", None, None),
        P("dom", None, None),
        P("dom"),
    )
    return jax.shard_map(
        on_device,
        mesh=mesh,
        in_specs=placed,
        out_specs=(P("band", None), P("band", None)),
        check_vma=False,
    )
```

```python
import jax
import jax.numpy as jnp
from jax import lax
from jax.experimental import pallas as pl
from jax.experimental.pallas import tpu as pltpu
from jax.sharding import PartitionSpec as P


F32 = jnp.float32
BF16 = jnp.bfloat16
HI = lax.Precision.HIGHEST
VMEM = pl.BlockSpec(memory_space=pltpu.VMEM)
SMEM = pl.BlockSpec(memory_space=pltpu.SMEM)


def lane_of(shape):
    return lax.broadcasted_iota(jnp.int32, shape, len(shape) - 1)


def turn(x, n):
    n = n % 128
    return pltpu.roll(x, n, 1) if n else x


MOVES = [(0, 0)] + [(y, z) for z in (4, 3, -3, 2, -2, 1, -1) for y in (0, 1)] + [(1, 0)]


def band_at(b, move, sign=1):
    return (b // 8 + move[0]) % 2 * 8 + (b + sign * move[1] + 8) % 8


def spread_kernel(wf, out, last, held, ready, sems):
    lane = lane_of((8, 128))
    block = lane // 8

    def fetch(i):
        rows = pl.ds(pl.multiple_of(i * 512, 512), 512)
        return pltpu.make_async_copy(wf.at[rows], held.at[rows], sems.at[i])

    for i in range(8):
        fetch(i).start()

    def body(bg, _):
        fetch(bg).wait()
        for x in range(4):
            v = [held[pl.ds(bg * 512 + x * 16 + y, 8, stride=64), :] for y in range(16)]
            for s in (1, 2, 4, 8):
                low = (block & s) == 0
                nxt = list(v)
                for y in range(16):
                    if not y & s:
                        a, b = v[y], v[y + s]
                        if s == 8:
                            a_high = b_low = turn(jnp.where(low, b, a), 64)
                        else:
                            b_low, a_high = turn(b, s * 8), turn(a, -s * 8)
                        nxt[y] = jnp.where(low, a, b_low)
                        nxt[y + s] = jnp.where(low, a_high, b)
                v = nxt
            rows = pl.ds(pl.multiple_of(x * 64 + bg * 8, 8), 8)
            for k in range(16):
                ready[k, rows, :] = v[k]
        return 0

    lax.fori_loop(0, 8, body, 0)
    one = pltpu.make_async_copy(ready.at[:, :192], out, sems.at[8])
    two = pltpu.make_async_copy(ready.at[:, 192:], last, sems.at[9])
    one.start()
    two.start()
    one.wait()
    two.wait()


def plane_kernel(r, out):
    out[...] = r[...]


def edge_kernel(r, below):
    lane = lane_of((32, 128))

    def body(g, _):
        acc = r[g, :32, :]
        for i in (1, 2, 4, 5, 6):
            at = i % 4 * 64 + i // 4 * 32
            acc = jnp.where(lane % 8 == i, turn(r[g, at : at + 32, :], i), acc)
        below[g] = acc
        return 0

    lax.fori_loop(0, 16, body, 0)


def split(x):
    hi = x.astype(BF16)
    return hi, (x - hi.astype(F32)).astype(BF16)


def dot(a, b):
    return lax.dot_general(a, b, (((1,), (1,)), ((), ())), preferred_element_type=F32)


def slots(e, er, i, j):
    return lax.dot_general(e[:, i], er[:, j], (((0,), (0,)), ((), ())), preferred_element_type=F32)


def place(g):
    return (g % 2) * 8 + g // 2


FIRST = (0, 8, 10)


def couple_kernel(hc, ds, out):
    lane = lane_of((24, 128))
    out[...] = jnp.zeros_like(out)
    for t, m in enumerate((hc, ds)):
        for a in range(4):
            out[t, a, :16, :18] = m[a, :16, :]
            out[t, a, 16:, :18] = m[a, 10:18, :]
            v = out[t, a]
            out[t, a] = jnp.where(lane < 16, v, jnp.where(lane < 24, turn(v, 6), jnp.zeros_like(v)))


def coef_kernel(ids, count, wf, proj, sym, potential, last, pot, *refs):
    outs, (rows, padded, plain) = refs[:16], refs[16:]
    for x in range(4):
        v = pltpu.roll(potential[x], lax.rem(128 - 8 * ids[0], 128), 1)
        own = lane_of((16, 128)) // 8 == lax.broadcasted_iota(jnp.int32, (16, 128), 0)
        v = jnp.where(own, pltpu.roll(v, 0, 1, stride=8, stride_axis=0), jnp.zeros_like(v))
        pot[x : x + 1, :] = jnp.sum(v, axis=0, keepdims=True)

    def add(i, acc):
        p, w = [], []
        for xy in (4 * i, 4 * i + 1, 4 * i + 2, 4 * i + 3):
            p.append(jnp.concatenate([proj[pl.ds((18 * a + f) * 64 + xy, 8, stride=64), :] for a in range(4) for f in FIRST], axis=0))
            w.append(wf[pl.ds(xy, 64, stride=64), :])
        ph, plo = split(jnp.concatenate(p, axis=1))
        wh, wlo = split(jnp.concatenate(w, axis=1))
        return acc + (dot(ph, wh) + dot(ph, wlo) + dot(plo, wh))

    acc = lax.fori_loop(0, 16, add, jnp.zeros((96, 64), F32))
    row = lax.broadcasted_iota(jnp.int32, (24, 64), 0)
    slot = jnp.where(row < 16, row, row - 6)
    rows[...] = jnp.zeros_like(rows)
    plain[...] = jnp.zeros_like(plain)
    for a in range(4):
        kept = (slot < count[a]) & ((row < 16) | (slot >= 16))
        c = jnp.where(kept, acc[a * 24 : a * 24 + 24], jnp.zeros((24, 64), F32))
        padded[...] = jnp.zeros_like(padded)
        padded[:24, :] = c
        found = [c]
        for t in range(2):
            m = sym[t, a]
            right = jnp.dot(m, padded[...], precision=HI, preferred_element_type=F32)
            left = lax.dot_general(m, c, (((0,), (0,)), ((), ())), precision=HI, preferred_element_type=F32)
            found.append(0.5 * (right + left[:24]))
        for t, v in enumerate(found):
            plain[t, 18 * a : 18 * a + 16, :] = v[:16]
            plain[t, 18 * a + 16 : 18 * a + 18, :] = v[22:]
    for k in range(16):
        own = slice(5 * k, 5 * k + 5)
        rows[k, 0:5, :64] = plain[0, own, :]
        rows[k, 5:8, :64] = plain[1, 5 * k : 5 * k + 3, :]
        rows[k, 0:2, 64:] = plain[1, 5 * k + 3 : 5 * k + 5, :]
        rows[k, 2:7, 64:] = plain[2, own, :]
    lane = lane_of((8, 128))
    for m, out in zip(MOVES, outs):
        to = band_at(ids[0], m)
        out[:8, :] = rows[to]
        out[16:, :] = last[to]
        after = lax.rem(to + 1, 16)
        acc = last[after, :8, :]
        for i in range(1, 8):
            acc = jnp.where(lane % 8 == i, turn(last[after, i * 8 : i * 8 + 8, :], i), acc)
        out[8:16, :] = acc


def corr_kernel(r, pot, ah, al, part, ce, co):
    volume = 1.0 / (512 * 256)
    lane = lane_of((64, 128))
    zero = jnp.zeros((64, 128), F32)

    def prepare(g, _):
        to = pl.ds(pl.multiple_of(place(g) * 64, 64), 64)
        for x in range(3):
            cols = slice(x * 128, (x + 1) * 128)
            p = r[g, x * 64 : (x + 1) * 64, :]
            ah[to, cols], al[to, cols] = split(p)
            beside = turn(p, -8) + jnp.where(lane % 8 == 7, zero, turn(p, -1))
            if x < 2:
                beside = beside + r[g, (x + 1) * 64 : (x + 2) * 64, :]
            part[to, cols] = (1.5 + 0.5 * pot[x : x + 1, :]) * p - 0.5 * beside
        return 0

    lax.fori_loop(0, 16, prepare, 0)

    def corr(i, j):
        i, j = slice(i, i + 256), slice(j, j + 256)
        acc = dot(ah[i, :], ah[j, :]) + dot(ah[i, :], al[j, :]) + dot(al[i, :], ah[j, :])
        return acc * volume

    for q in range(2):
        for n, (i, j) in enumerate(((0, 0), (256, 0), (256, 256))):
            ce[q, n] = corr(q * 512 + i, q * 512 + j)
    for i in (0, 256):
        for j in (0, 256):
            co[i : i + 256, j : j + 256] = corr(512 + i, j)


def gram(which, ah, al, ph, lo, er, eh, ce, co, out, c, on):
    low = lane_of((64, 128)) < 64

    def ham(i, j):
        i, j = slice(i, i + 256), slice(j, j + 256)
        acc = dot(ph[i, :], ah[j, :]) + dot(ph[i, :], al[j, :]) + dot(lo[i, :], ah[j, :])
        acc += dot(ah[i, :], ph[j, :]) + dot(al[i, :], ph[j, :]) + dot(ah[i, :], lo[j, :])
        return acc + slots(eh, er, i, j)

    def tiles(e, f, t, get):
        for j in range(4):
            if f % 2:
                lower, upper = get(2 * j + 1, (f - 2 * j - 1) % 8 // 2), get(2 * j, (f - 2 * j - 1) % 8 // 2)
            else:
                lower, upper = get(2 * j, (f - 2 * j) % 8 // 2), get(2 * j + 1, (f - 2 * j - 2) % 8 // 2)
            out[e, (t + j) * 64 : (t + j) * 64 + 64, :] = jnp.where(low, lower, upper)

    @pl.when(which == 0)
    def _():
        row = lax.broadcasted_iota(jnp.int32, (256, 256), 0)
        col = lax.broadcasted_iota(jnp.int32, (256, 256), 1)
        for q in range(2):
            at = q * 512
            c[q, :256, 256:] = ham(at, at + 256)
            c[q, 256:, :256] = ce[q, 1]
            for n in range(2):
                here, own = slice(n * 256, n * 256 + 256), ce[q, 2 * n]
                c[q, here, here] = jnp.where(row <= col, ham(at + n * 256, at + n * 256), own)
                diagonal = jnp.sum(jnp.where(row == col, own, jnp.zeros_like(own)), axis=0, keepdims=True)
                on[q, n] = jnp.broadcast_to(diagonal, (8, 256))
        for e in range(8):
            for q in range(2):
                tiles(e, (e - q) % 8, q * 4, lambda m, n: c[q, m * 64 : m * 64 + 64, n * 128 : n * 128 + 128])
            m = e // 2
            cols = slice(m // 2 * 128, m // 2 * 128 + 128)
            a, b = on[e % 2, 0, :, cols], on[e % 2, 1, :, cols]
            if m % 2:
                a = turn(a, 64)
            else:
                b = turn(b, 64)
            out[e, 512:, :] = jnp.where(low[:8], a, b)

    @pl.when(which == 1)
    def _():
        for i in (0, 256):
            for j in (0, 256):
                c[0, i : i + 256, j : j + 256] = ham(i, 512 + j)
        for e in range(8):
            tiles(e, e, 0, lambda m, n: c[0, m * 64 : m * 64 + 64, n * 128 : n * 128 + 128])
            tiles(e, e, 4, lambda m, n: co[m * 64 : m * 64 + 64, n * 128 : n * 128 + 128])
            out[e, 512:, :] = jnp.zeros((8, 128), F32)


def fourth_kernel(ids, pot, three, th, tl, fe, fo, *refs):
    came, (ah, al, part, er, eh, es, ce, co, last, cc) = refs[:16], refs[16:]
    volume = 1.0 / (512 * 256)
    lane = lane_of((64, 128))
    for m, v in zip(MOVES, came):
        g = band_at(ids[0], m, -1)
        cc[g] = v[:8, :]
        last[g] = v[8:, :]
    half = lane_of((8, 128)) < 64
    none = jnp.zeros((3, 128), F32)
    for n in range(8):
        a, b = cc[4 * n % 16 + n // 4], cc[(4 * n + 2) % 16 + n // 4]
        x, y = jnp.where(half, a, turn(b, 64)), jnp.where(half, turn(a, 64), b)
        for t, (e, v) in enumerate(((er, x[:5]), (eh, jnp.concatenate([x[5:], y[:2]], axis=0)), (es, y[2:7]))):
            hi, mid = [w.astype(F32) for w in split(jnp.concatenate([v, none], axis=0))]
            zero = jnp.zeros_like(hi)
            terms = [hi, hi, mid, zero] if t else [hi, mid, hi, zero]
            e[:, n * 128 : n * 128 + 128] = jnp.concatenate(terms, axis=0).astype(BF16)

    def prepare(g, _):
        to = pl.ds(pl.multiple_of(place(g) * 64, 64), 64)
        p = last[g, 8:, :]
        ah[to, :384], al[to, :384] = th[to, :], tl[to, :]
        ah[to, 384:], al[to, 384:] = split(p)
        part[to, :256] = three[to, :256]
        part[to, 256:384] = three[to, 256:] - 0.5 * p
        after = last[g, :8, :]
        after = jnp.concatenate([turn(after, 7 - i) for i in range(8)], axis=0)
        beside = turn(p, -8) + jnp.where(lane % 8 == 7, after, turn(p, -1))
        part[to, 384:] = (1.5 + 0.5 * pot[3:4, :]) * p - 0.5 * beside
        return 0

    lax.fori_loop(0, 16, prepare, 0)

    def corr(v, i, j):
        i, j, x = slice(i, i + 256), slice(j, j + 256), slice(384, 512)
        acc = dot(ah[i, x], ah[j, x]) + dot(ah[i, x], al[j, x]) + dot(al[i, x], ah[j, x])
        return v + acc * volume + slots(es, er, i, j)

    for q in range(2):
        for n, (i, j) in enumerate(((0, 0), (256, 0), (256, 256))):
            ce[q, n] = corr(fe[q, n], q * 512 + i, q * 512 + j)
    for i in (0, 256):
        for j in (0, 256):
            co[i : i + 256, j : j + 256] = corr(fo[i : i + 256, j : j + 256], 512 + i, j)


def send_kernel(ids, part, xh, zh, ah, al, er, eh, ce, co, out, ph, lo, c, on):
    volume = 1.0 / (512 * 256)
    lane = lane_of((64, 128))

    def prepare(g, _):
        to = pl.ds(pl.multiple_of(place(g) * 64, 64), 64)
        two = zh[g]
        ext = jnp.concatenate([two, turn(two, -4)], axis=0)
        for x in range(4):
            cols = slice(x * 128, (x + 1) * 128)
            beside = jnp.where(lane % 8 == 7, turn(ext, 7 - x), jnp.zeros((64, 128), F32)) if x < 3 else xh[g]
            ph[to, cols], lo[to, cols] = split((part[to, cols] - 0.5 * beside) * volume)
        return 0

    lax.fori_loop(0, 16, prepare, 0)
    gram(1 - lax.rem(ids[1], 2), ah, al, ph, lo, er, eh, ce, co, out, c, on)


def keep_kernel(ids, ph, lo, ah, al, er, eh, ce, co, out, c, on):
    gram(lax.rem(ids[1], 2), ah, al, ph, lo, er, eh, ce, co, out, c, on)


def first_kernel(ids, keep, mate, s1, s2, s3, own):
    d = ids[1]
    north, x, h = lax.rem(d, 2) == 1, d // 4, lax.rem(d // 2, 2)

    def total(ref, i, across, along):
        e = jnp.where(north, along, across)
        ref[i] = keep[e] + mate[e]

    def part(dx, y):
        return lax.rem(x + dx, 4) * 2 + y

    for i in range(2):
        total(s1, i, part(1, i), part(i, 1 - h))
        total(s2, i, part(3, i), part(2 + i, 1 - h))
        total(own, i, part(0, i), part(i, h))
        total(own, 2 + i, part(0, i), part(2 + i, h))
        total(s3, i, part(2, i), part(2, i))


def second_kernel(ids, own, r1, r2, r3, keep, s1, s2, s3):
    d = ids[1]
    north, h = lax.rem(d, 2) == 1, lax.rem(d // 2, 2)

    @pl.when(jnp.logical_not(north))
    def _():
        def total(i):
            return own[i] + r1[i] + r2[i] + r3[i]

        keep[...] = total(h)
        s1[...] = total(1 - h)

    @pl.when(north)
    def _():
        keep[...] = own[0] + r1[0]
        s1[...] = own[1] + r1[1]
        s3[...] = own[2] + r2[0]
        s2[...] = own[3] + r2[1]


def rows_kernel(ids, keep, r1, r2, r3, out, total):
    d = ids[1]
    low = lane_of((64, 128)) < 64
    total[...] = keep[...] + r1[...]

    @pl.when(lax.rem(d, 2) == 1)
    def _():
        total[...] = total[...] + (r2[...] + r3[...])

    e = d // 2
    even = 1 - lax.rem(d, 2)

    def block(g, upper):
        m, p = g // 2, lax.rem(g, 2)
        t = total[pl.ds(pl.multiple_of((p * 4 + m // 2) * 64, 64), 64), :]
        half = lax.rem(m + e + even * p, 2)
        return jnp.where(half == upper, t, pltpu.roll(t, 64, 1))

    for g in range(16):
        h = lax.rem(d - g + 16, 16)
        own = jnp.broadcast_to(total[512:513, :], (64, 128))
        own = own if g >= 8 else turn(own, 64)
        out[g] = jnp.where(low, block(jnp.int32(g), 0), jnp.where(h == g, own, block(h, 1)))


def finish_kernel(ids, parts, out):
    b, d = ids[0], ids[1]
    h = lax.rem(d - b + 16, 16)
    t = parts[0]
    for s in range(1, 16):
        t = t + parts[s]
    low = lane_of((64, 128)) < 64
    both = jnp.concatenate([t, t], axis=0).T
    left, right, other = both[:64], both[64:], turn(t, 64)
    upper = jnp.where(low, t, right)
    lower = jnp.where(low, right, other)
    row, col = lax.broadcasted_iota(jnp.int32, (64, 128), 0), lane_of((64, 128)) % 64
    own = jnp.where(low, jnp.where(row <= col, t, left), jnp.where(row > col, other, jnp.where(row < col, left, t)))
    first = jnp.where(lax.rem(d, 2) == 1, lax.rem(b, 2), (b > h).astype(jnp.int32)) == 0
    out[...] = jnp.where(b == h, own, jnp.where(first, upper, lower))


def join_kernel(a, b, c, d, out):
    for i, v in enumerate((a, b, c, d)):
        out[i] = v[...]


def assemble_kernel(ids, own, r1, r2, r3, ham, corr, parts):
    b, d = ids[0], ids[1]
    low = lane_of((64, 128)) < 64
    for i, v in enumerate((own, r1, r2, r3)):
        parts[4 * i : 4 * i + 4] = v[...]

    def piece(h):
        at = lax.rem(h + b, 16)
        ahead = lax.rem(at // 4 - d // 4 + 4, 4)
        return parts[ahead * 4 + (lax.rem(at, 4) ^ lax.rem(d, 4))]

    for j in range(8):
        t0, t1 = piece(2 * j), piece(2 * j + 1)
        cols = slice(j * 128, (j + 1) * 128)
        ham[:, cols] = jnp.where(low, t0, turn(t1, 64))
        corr[:, cols] = jnp.where(low, turn(t0, 64), t1)


def call(kernel, args, outs, scratch=(), flops=0, mib=8):
    specs = [SMEM if a.dtype == jnp.int32 else VMEM for a in args]
    size = sum(a.size * a.dtype.itemsize for a in (*args, *outs))
    single = len(outs) == 1
    return pl.pallas_call(
        kernel,
        out_shape=outs[0] if single else outs,
        in_specs=specs,
        out_specs=VMEM if single else [VMEM] * len(outs),
        scratch_shapes=scratch,
        compiler_params=pltpu.CompilerParams(vmem_limit_bytes=mib * 1024 * 1024),
        cost_estimate=pl.CostEstimate(flops=flops or 8 * size, bytes_accessed=size, transcendentals=0),
    )(*args)


def shape(*dims, dtype=F32):
    return jax.ShapeDtypeStruct(dims, dtype)


def moves(south, north):
    pairs = []
    for d in range(16):
        x, h, c = d // 4, d // 2 % 2, d % 2
        step = north if c else south
        if step:
            pairs.append((d, (x + step[0]) % 4 * 4 + (h + step[1]) % 2 * 2 + c))
    return pairs


def reduced_over_dom(ids, keep, mate):
    piece = (520, 128)
    sends = call(first_kernel, (ids, keep, mate), [shape(n, *piece) for n in (2, 2, 2, 4)], mib=16)
    steps = (((1, 0), (0, 1)), ((3, 0), (0, 1)), ((2, 0), None))
    got = [lax.ppermute(v, "dom", moves(*s)) for v, s in zip(sends, steps)]
    keep, *sends = call(second_kernel, (ids, sends[3], *got), [shape(*piece)] * 4, mib=12)
    steps = (((0, 1), (1, 0)), (None, (3, 0)), (None, (2, 0)))
    got = [lax.ppermute(v, "dom", moves(*s)) for v, s in zip(sends, steps)]
    return call(rows_kernel, (ids, keep, *got), (shape(16, 64, 128),), [pltpu.VMEM(piece, F32)], mib=8)


def on_device(wavefunctions, potential, projectors, hamiltonian_correction, delta_s, projector_count):
    bands, cx, ny, nz = wavefunctions.shape
    atoms, slots = hamiltonian_correction.shape[:2]
    b, d = lax.axis_index("band"), lax.axis_index("dom")
    ids = jnp.stack([b, d]).astype(jnp.int32)

    flat = cx * ny
    wf = wavefunctions.reshape(bands * flat, nz)
    parts, last = pl.pallas_call(
        spread_kernel,
        out_shape=[shape(16, 3 * bands, 128), shape(16, bands, 128)],
        in_specs=[pl.BlockSpec(memory_space=pltpu.HBM)],
        out_specs=[pl.BlockSpec(memory_space=pltpu.HBM)] * 2,
        scratch_shapes=[
            pltpu.VMEM((bands * flat, nz), F32),
            pltpu.VMEM((16, cx * bands, 128), F32),
            pltpu.SemaphoreType.DMA((10,)),
        ],
        compiler_params=pltpu.CompilerParams(vmem_limit_bytes=61 * 1024 * 1024),
    )(wf)
    slab = lax.all_to_all(parts, "band", 0, 0, tiled=True)

    proj = projectors.reshape(atoms * slots * flat, nz)
    wf, proj, potential, hamiltonian_correction, delta_s, parts = lax.optimization_barrier(
        (wf, proj, potential, hamiltonian_correction, delta_s, parts)
    )
    sym = call(couple_kernel, (hamiltonian_correction, delta_s), (shape(2, atoms, 24, 128),), mib=2)
    pot, *came = call(
        coef_kernel,
        (ids, projector_count, wf, proj, sym, potential, last),
        [shape(cx, nz)] + [shape(16 + bands, 128)] * 16,
        [pltpu.VMEM((16, 8, 128), F32), pltpu.VMEM((128, bands), F32), pltpu.VMEM((3, 80, bands), F32)],
    )
    for i, move in enumerate(MOVES):
        if i:
            came[i] = lax.ppermute(came[i], "band", [(j, band_at(j, move)) for j in range(16)])
    back = [((i + 1) % 16, i) for i in range(16)]
    first = pl.pallas_call(
        plane_kernel,
        grid=(1,),
        out_shape=shape(16, bands, 128),
        in_specs=[pl.BlockSpec((16, bands, 128), lambda i: (0, 0, 0))],
        out_specs=pl.BlockSpec((16, bands, 128), lambda i: (0, 0, 0)),
        compiler_params=pltpu.CompilerParams(vmem_limit_bytes=4 * 1024 * 1024),
        cost_estimate=pl.CostEstimate(flops=1000, bytes_accessed=2**20, transcendentals=0),
    )(slab)
    below = call(edge_kernel, (slab,), [shape(16, bands // 2, 128)], mib=4)
    ahead, above = lax.ppermute(first, "dom", back), lax.ppermute(below, "band", back)
    m = 16 * bands
    three, wide = shape(m, 384, dtype=BF16), shape(m, 512, dtype=BF16)
    ext = [shape(32, m, dtype=BF16)] * 3
    work = 2 * m * m * 512
    quads = [pltpu.VMEM((2, 512, 512), F32), pltpu.VMEM((2, 2, 8, 256), F32)]
    ah, al, part, ce, co = call(
        corr_kernel,
        (slab, pot),
        [three, three, shape(m, 384), shape(2, 3, 256, 256), shape(512, 512)],
        flops=3 * work,
        mib=16,
    )
    ah, *came = lax.optimization_barrier((ah, *came))
    parts = shape(8, 520, 128)
    ah, al, part, er, eh, _, ce, co = call(
        fourth_kernel,
        (ids, pot, part, ah, al, ce, co, *came),
        [wide, wide, shape(m, 512), *ext, shape(2, 3, 256, 256), shape(512, 512)],
        [pltpu.VMEM((16, 72, 128), F32), pltpu.VMEM((16, 8, 128), F32)],
        2 * work,
        20,
    )
    corr = (ah, al, er, eh, ce, co)
    ahead, above, corr = lax.optimization_barrier((ahead, above, corr))
    send, ph, lo = call(send_kernel, (ids, part, ahead, above, *corr), [parts, wide, wide], quads, 3 * work, 20)
    mate = lax.ppermute(send, "dom", [(i, i ^ 1) for i in range(16)])
    keep = call(keep_kernel, (ids, ph, lo, *corr), [parts], quads, 3 * work, 18)
    parts = reduced_over_dom(ids, keep, mate)
    parts = lax.all_to_all(parts, "band", 0, 0, tiled=True)
    own = call(finish_kernel, (ids, parts), (shape(64, 128),))
    near = [lax.ppermute(own, "dom", [(i, i ^ j) for i in range(16)]) for j in (1, 2, 3)]
    own = call(join_kernel, (own, *near), (shape(4, 64, 128),))
    far = [lax.ppermute(own, "dom", [((i + 4 * j) % 16, i) for i in range(16)]) for j in (1, 2, 3)]
    return call(
        assemble_kernel,
        (ids, own, *far),
        (shape(64, 1024), shape(64, 1024)),
        [pltpu.VMEM((16, 64, 128), F32)],
    )


def solution(mesh):
    placed = (
        P("band", "dom", None, None),
        P("dom", None, None),
        P("dom", None, None, None, None),
        P("dom", None, None),
        P("dom", None, None),
        P("dom"),
    )
    return jax.shard_map(
        on_device,
        mesh=mesh,
        in_specs=placed,
        out_specs=(P("band", None), P("band", None)),
        check_vma=False,
    )
```
